256 devices in a mesh: cfg: 2 (over y), ta: 16 (over z), xyz: 8 (over x, core).
Axes of the slice: x: 4, y: 2, z: 16, core: 2. Of those that a mesh axis runs over, the one named last changes fastest.
The devices are a block of a 4x16x16 slice.
Arguments:
- sink: float32 [24, 4, 3, 2, 16, 64, 128], P('cfg', None, None, None, 'ta', 'xyz'), parts along dimension 0, may hold values from -6 to 6
- links: float32 [16, 4, 3, 3, 2, 16, 64, 128], P('cfg', None, None, None, None, 'ta', 'xyz'), parts along dimension 0, may hold values from -2 to 2
- section_index: int32 [2, 3], replicated, may hold values from 0 to 7
- momenta: int32 [33, 3], replicated, may hold values from -3 to 3
- source: int32 [3], replicated, may hold values from 0 to 15
Outputs:
- adjoint: float32 [24, 4, 3, 2, 16, 64, 128], P('cfg', None, None, None, 'ta', 'xyz'), parts along dimension 0
- correlator: float32 [4, 33, 16], P('cfg', None, 'ta'), parts along dimension 0
The draws below stay inside these ranges and needn't reach their ends.
There are 2 independent parts, one for each index of `cfg`. The reference program is written for one: setup_inputs(seed, part) draws one part's arguments, and reference() takes and returns one part's arrays. A program takes and returns all parts, laid end to end along the dimension named above; an argument that names none is the same for every part. Nothing has to cross between parts.
All inputs are finite; a program needn't handle non-finite values.
Results may differ from the reference program's by a relative error of at most 0.000068.
Values sent between devices are 32-bit elements; how exact they have to be, the bound alone decides.
No kernel may reach another device: no remote copies, remote signals or barrier semaphores. Data moves between devices by JAX's collectives and lax.ppermute only.
A program may use at most 128 MiB of HBM per device.

```python
import math
import jax
import jax.numpy as jnp
from jax import lax

NCOL = 12
NMOM = 33
STEPS = 2
SLOTS = 8
LY = 16
NT = 16
NX = 64
NY = 16
NZ = 8


def touch_ends(drawn, rng, least, largest):
    dims = drawn.shape
    index_at = [jax.random.randint(jax.random.fold_in(rng, axis), (), 0, dims[axis]) for axis in range(len(dims))]
    drawn = drawn.at[tuple(index_at)].set(least)
    longest = dims.index(max(dims))
    index_at[longest] = (index_at[longest] + 1) % dims[longest]
    return drawn.at[tuple(index_at)].set(largest)


def block_scale(stream_key, shape, cuts, smallest, high):
    loudness = 1.0
    for position, blocks in cuts:
        draws = jax.random.uniform(jax.random.fold_in(jax.random.fold_in(stream_key, 6), position), (blocks,), jnp.float32, smallest / len(cuts), high / len(cuts))
        loudness = loudness * jnp.repeat(jnp.exp(draws), shape[position] // blocks).reshape((-1,) + (1,) * (len(shape) - 1 - position))
    return loudness


def bell_draw(rng, dims, spread, reach, pieces=(), held_as=jnp.bfloat16):
    result = jax.random.normal(rng, dims, jnp.float32) * spread
    if len(pieces) > 0:
        result = block_scale(rng, dims, pieces, -0.22, 0.18) * result
    return jnp.clip(result, min=-reach, max=reach).astype(held_as)


def setup_inputs(seed: int = 0, part: int = 0) -> dict:
    seeds = jax.random.split(jax.random.key(seed), 6)
    own_keys = jax.random.split(jax.random.fold_in(seeds[5], part), 6)
    return {
        "sink": bell_draw(own_keys[0], (NCOL, 4, 3, 2, NT, NX, NY * NZ), 1.0, 6.0, ((4, 16), (5, 8)), jnp.float32),
        "links": bell_draw(own_keys[1], (SLOTS, 4, 3, 3, 2, NT, NX, NY * NZ), 0.35, 2.0, ((5, 16), (6, 8)), jnp.float32),
        "section_index": touch_ends(jax.random.randint(seeds[2], (STEPS, 3), 0, SLOTS), jax.random.fold_in(seeds[2], 1), 0, SLOTS - 1).astype(jnp.int32),
        "momenta": touch_ends(jax.random.randint(seeds[3], (NMOM, 3), -3, 4), jax.random.fold_in(seeds[3], 1), -3, 3).astype(jnp.int32),
        "source": jax.random.randint(seeds[4], (3,), 0, LY).astype(jnp.int32),
    }


flow_step = 0.05

def hop_forward(matrix, field):
    spin_real = field[:, :, :, 0]
    spin_imag = field[:, :, :, 1]
    terms_real = []
    terms_imag = []
    for colour in range(3):
        link_real = matrix[:, colour, 0][None, None]
        link_imag = matrix[:, colour, 1][None, None]
        part_real = spin_real[:, :, colour][:, :, None]
        part_imag = spin_imag[:, :, colour][:, :, None]
        terms_real.append(link_real * part_real - link_imag * part_imag)
        terms_imag.append(link_real * part_imag + link_imag * part_real)
    return jnp.stack([terms_real[0] + terms_real[1] + terms_real[2], terms_imag[0] + terms_imag[1] + terms_imag[2]], axis=3)

def hop_backward(matrix, field):
    spin_real = field[:, :, :, 0]
    spin_imag = field[:, :, :, 1]
    terms_real = []
    terms_imag = []
    for colour in range(3):
        link_real = matrix[colour, :, 0][None, None]
        link_imag = matrix[colour, :, 1][None, None]
        part_real = spin_real[:, :, colour][:, :, None]
        part_imag = spin_imag[:, :, colour][:, :, None]
        terms_real.append(link_real * part_real + link_imag * part_imag)
        terms_imag.append(link_real * part_imag - link_imag * part_real)
    return jnp.stack([terms_real[0] + terms_real[1] + terms_real[2], terms_imag[0] + terms_imag[1] + terms_imag[2]], axis=3)

def shift_inner(field, amount):
    zcoord = jnp.arange(NY * NZ, dtype=jnp.int32) % NZ
    if amount < 0:
        inside = jnp.roll(field, -1, axis=-1)
        wrapped = jnp.roll(field, NZ - 1, axis=-1)
        return jnp.where(zcoord == NZ - 1, wrapped, inside)
    inside = jnp.roll(field, 1, axis=-1)
    wrapped = jnp.roll(field, 1 - NZ, axis=-1)
    return jnp.where(zcoord == 0, wrapped, inside)

def roll_lattice(field, direction, amount):
    if direction == 0:
        return jnp.roll(field, amount, axis=-3)
    if direction == 1:
        return jnp.roll(field, amount, axis=-2)
    if direction == 2:
        return jnp.roll(field, amount * NZ, axis=-1)
    return shift_inner(field, amount)

def laplacian(field, section_links):
    total = -8.0 * field
    for direction in range(4):
        matrix = section_links[direction]
        total = total + hop_forward(matrix, roll_lattice(field, direction, -1))
        total = total + roll_lattice(hop_backward(matrix, field), direction, 1)
    return total

def adjoint_step(lam, first, second, third):
    coef_third = 0.75 * flow_step
    coef_second = 8.0 * flow_step / 9.0
    coef_first = 0.25 * flow_step
    coef_mixed = 2.0 * flow_step / 9.0
    later = coef_third * laplacian(lam, third)
    middle = lam + coef_second * laplacian(later, second)
    return middle + later + laplacian(coef_first * middle - coef_mixed * later, first)

def phase_table(xcoord, nx_total, momenta, source):
    plane_index = jnp.arange(NY * NZ, dtype=jnp.int32)
    ycoord = plane_index // NZ
    zcoord = plane_index % NZ
    dist_x = jnp.mod(xcoord - source[0], nx_total)
    dist_y = jnp.mod(ycoord - source[1], NY)
    dist_z = jnp.mod(zcoord - source[2], NZ)
    frac_x = jnp.mod(momenta[:, 0:1] * dist_x[None, :], nx_total).astype(jnp.float32) / float(nx_total)
    frac_y = jnp.mod(momenta[:, 1:2] * dist_y[None, :], NY).astype(jnp.float32) / float(NY)
    frac_z = jnp.mod(momenta[:, 2:3] * dist_z[None, :], NZ).astype(jnp.float32) / float(NZ)
    frac = frac_x[:, :, None] + frac_y[:, None, :] + frac_z[:, None, :]
    angle = 2.0 * math.pi * frac
    table = jnp.concatenate([jnp.cos(angle), -jnp.sin(angle)], axis=0)
    return table.reshape(2 * NMOM, xcoord.shape[0] * NY * NZ)

def reference(sink, links, section_index, momenta, source):
    lam = sink
    for step in reversed(range(STEPS)):
        sections = [lax.dynamic_index_in_dim(links, section_index[step, section], 0, keepdims=False) for section in range(3)]
        lam = adjoint_step(lam, sections[0], sections[1], sections[2])
    squares = lax.optimization_barrier(jnp.sum(lam * lam, axis=(0, 2, 3)))
    density = squares[0] + squares[1] - squares[2] - squares[3]
    density = density.reshape(NT, NX * NY * NZ)
    table = phase_table(jnp.arange(NX, dtype=jnp.int32), NX, momenta, source)
    projected = jnp.dot(density, table.T, precision=lax.Precision.HIGHEST)
    scale = 1.0 / math.sqrt(576.0 * NX * NY * NZ)
    projected = projected * scale
    correlator = jnp.transpose(projected.reshape(NT, 2, NMOM), (1, 2, 0))
    return (lam, correlator)
```

```python
import functools
import math

import jax
import jax.numpy as jnp
from jax import lax
from jax.experimental import pallas as pl
from jax.experimental.pallas import tpu as pltpu
from jax.sharding import PartitionSpec as P

NY = 16
NZ = 8
TILES = 24
CHUNKS = (6, 6)
VMEM_LIMIT = 16 * 1024 * 1024


flow_step = 0.05
coef_third = 0.75 * flow_step
coef_second = 8.0 * flow_step / 9.0
coef_first = 0.25 * flow_step
coef_mixed = 2.0 * flow_step / 9.0


def link_tile(ref, direction, row, column):
    at = ((direction * 3 + row) * 3 + column) * 2
    return ref[0, at], ref[0, at + 1]


def forward(ref, direction, vector):
    out = []
    for row in range(3):
        real = imag = None
        for column in range(3):
            wr, wi = link_tile(ref, direction, row, column)
            vr, vi = vector[column]
            re = wr * vr - wi * vi
            im = wr * vi + wi * vr
            real = re if real is None else real + re
            imag = im if imag is None else imag + im
        out.append((real, imag))
    return out


def backward(ref, direction, vector):
    out = []
    for row in range(3):
        real = imag = None
        for column in range(3):
            wr, wi = link_tile(ref, direction, column, row)
            vr, vi = vector[column]
            re = wr * vr + wi * vi
            im = wr * vi - wi * vr
            real = re if real is None else real + re
            imag = im if imag is None else imag + im
        out.append((real, imag))
    return out


def each(function, *vectors):
    return [
        tuple(function(*(vector[colour][part] for vector in vectors)) for part in range(2))
        for colour in range(3)
    ]


def tiles_of(ref, base):
    return [(ref[base + 2 * colour], ref[base + 2 * colour + 1]) for colour in range(3)]


def rows_of(ref, base):
    return [
        tuple(
            jnp.broadcast_to(ref[pl.ds(base + 2 * colour + part, 1), :], (8, 128))
            for part in range(2)
        )
        for colour in range(3)
    ]


def put_tiles(ref, base, vector):
    for colour in range(3):
        for part in range(2):
            ref[base + 2 * colour + part] = vector[colour][part]


def put_rows(ref, base, vector, row):
    for colour in range(3):
        for part in range(2):
            ref[pl.ds(base + 2 * colour + part, 1), :] = vector[colour][part][row : row + 1, :]


def roll(value, shift, axis):
    return pltpu.roll(value, shift % value.shape[axis], axis)


def messages(next_ref, base, field, pulled_ref, low_ref, high_ref):
    put_tiles(pulled_ref, base, backward(next_ref, 0, field))
    put_rows(low_ref, base, field, 0)
    put_rows(high_ref, base, backward(next_ref, 1, field), 7)


def first_kernel(index_ref, field_ref, next_ref, pulled_ref, low_ref, high_ref):
    for spin in range(4):
        base = 6 * spin
        messages(next_ref, base, tiles_of(field_ref, base), pulled_ref, low_ref, high_ref)


def lap_kernel(kind, last, index_ref, *refs):
    refs = list(refs)
    centre_ref, above_ref, below_ref, right_ref, left_ref, link_ref = refs[:6]
    refs = refs[6:]
    aux_ref = refs.pop(0) if kind > 0 else None
    if last:
        if len(refs) == 3:
            refs.pop(0)
        out_ref, density_ref = refs
    else:
        next_ref, out_ref = refs[:2]
        refs = refs[2:]
        sum_ref = refs.pop(0) if kind == 1 else None
        pulled_ref, low_ref, high_ref = refs

    sub = lax.broadcasted_iota(jnp.int32, (8, 128), 0)
    zcoord = lax.broadcasted_iota(jnp.int32, (8, 128), 1) % NZ
    is_top, is_bottom = sub == 7, sub == 0
    is_far, is_near = zcoord == NZ - 1, zcoord == 0
    density = None
    for spin in range(4):
        base = 6 * spin
        centre = tiles_of(centre_ref, base)
        total = each(lambda v, p: p - 8.0 * v, centre, tiles_of(below_ref, base))
        add = functools.partial(each, lambda a, b: a + b)
        total = add(total, forward(link_ref, 0, tiles_of(above_ref, base)))
        total = add(
            total,
            forward(
                link_ref,
                1,
                each(
                    lambda v, h: jnp.where(is_top, h, roll(v, -1, 0)),
                    centre,
                    rows_of(right_ref, base),
                ),
            ),
        )
        total = add(
            total,
            each(
                lambda v, h: jnp.where(is_bottom, h, roll(v, 1, 0)),
                backward(link_ref, 1, centre),
                rows_of(left_ref, base),
            ),
        )
        total = add(total, forward(link_ref, 2, each(lambda v: roll(v, -NZ, 1), centre)))
        total = add(total, each(lambda v: roll(v, NZ, 1), backward(link_ref, 2, centre)))
        total = add(
            total,
            forward(
                link_ref,
                3,
                each(lambda v: jnp.where(is_far, roll(v, NZ - 1, 1), roll(v, -1, 1)), centre),
            ),
        )
        total = add(
            total,
            each(
                lambda v: jnp.where(is_near, roll(v, 1 - NZ, 1), roll(v, 1, 1)),
                backward(link_ref, 3, centre),
            ),
        )
        if kind == 0:
            field = each(lambda t: coef_third * t, total)
        elif kind == 1:
            middle = each(lambda a, t: a + coef_second * t, tiles_of(aux_ref, base), total)
            field = each(lambda m, v: coef_first * m - coef_mixed * v, middle, centre)
            put_tiles(sum_ref, base, add(middle, centre))
        else:
            field = add(tiles_of(aux_ref, base), total)
        put_tiles(out_ref, base, field)
        if last:
            part = None
            for colour in range(3):
                for value in field[colour]:
                    part = value * value if part is None else part + value * value
            if density is None:
                density = part
            elif spin < 2:
                density = density + part
            else:
                density = density - part
        else:
            messages(next_ref, base, field, pulled_ref, low_ref, high_ref)
    if last:

        @pl.when(pl.program_id(0) == 0)
        def _():
            density_ref[...] = density

        @pl.when(pl.program_id(0) > 0)
        def _():
            density_ref[...] = density_ref[...] + density


def field_spec(offset):
    return pl.BlockSpec((TILES, 8, 128), lambda i, index: (i + offset, 0, 0))


def rows_spec():
    return pl.BlockSpec((TILES, 128), lambda i, index: (i, 0))


def links_spec(lap, tiles):
    return pl.BlockSpec((1, tiles, 8, 128), lambda i, index: (index[lap], 0, 0, 0))


def shape(*dims):
    return jax.ShapeDtypeStruct(dims, jnp.float32)


def cost(columns, per_spin, arrays):
    return pl.CostEstimate(
        flops=columns * 4 * per_spin * 1024,
        bytes_accessed=columns * TILES * 4096 * arrays,
        transcendentals=0,
    )


def first_messages(index, links, field, offset, columns):
    return pl.pallas_call(
        first_kernel,
        grid_spec=pltpu.PrefetchScalarGridSpec(
            num_scalar_prefetch=1,
            grid=(columns,),
            in_specs=[field_spec(offset), links_spec(0, 36)],
            out_specs=[field_spec(0), rows_spec(), rows_spec()],
        ),
        out_shape=[
            shape(columns * TILES, 8, 128),
            shape(columns * TILES, 128),
            shape(columns * TILES, 128),
        ],
        compiler_params=pltpu.CompilerParams(vmem_limit_bytes=VMEM_LIMIT),
        cost_estimate=cost(columns, 140, 2),
        name="first_messages",
    )(index, field, links)


def lap_call(lap, index, links, centre, arrived, aux, columns, whole=None):
    kind = lap % 3
    last = whole is not None
    above, below, right, left = arrived
    operands = [centre[0], above, below, right, left, links]
    in_specs = [
        field_spec(centre[1]),
        field_spec(0),
        field_spec(0),
        rows_spec(),
        rows_spec(),
        links_spec(lap, 72),
    ]
    if kind > 0:
        operands.append(aux[0])
        in_specs.append(field_spec(aux[1]))
    aliases = {}
    if last:
        before, every, buffer = whole
        if buffer is not None:
            aliases = {len(operands) + 1: 0}
            operands.append(buffer)
            in_specs.append(pl.BlockSpec(memory_space=pl.ANY))
        out_specs = [field_spec(before), pl.BlockSpec((8, 128), lambda i, index: (0, 0))]
        out_shape = [shape(every * TILES, 8, 128), shape(8, 128)]
    else:
        operands.append(links)
        in_specs.append(links_spec(lap + 1, 36))
        fields = 3 if kind == 1 else 2
        out_specs = [field_spec(0)] * fields + [rows_spec()] * 2
        out_shape = [shape(columns * TILES, 8, 128)] * fields + [shape(columns * TILES, 128)] * 2
    return pl.pallas_call(
        functools.partial(lap_kernel, kind, last),
        grid_spec=pltpu.PrefetchScalarGridSpec(
            num_scalar_prefetch=1,
            grid=(columns,),
            in_specs=in_specs,
            out_specs=out_specs,
        ),
        out_shape=out_shape,
        input_output_aliases=aliases,
        compiler_params=pltpu.CompilerParams(vmem_limit_bytes=VMEM_LIMIT),
        cost_estimate=cost(columns, 700, 6),
        name=f"lap{lap}_{columns}",
    )(index, *operands)


def passed_along(block, axis, distance):
    devices = range(lax.axis_size(axis))
    route = [((i - distance) % len(devices), i) for i in devices]
    return lax.ppermute(block, axis, route)


def exchanged(field, pulled, low, high):
    return (
        passed_along(field, "ta", -1),
        passed_along(pulled, "ta", 1),
        passed_along(low, "xyz", -1),
        passed_along(high, "xyz", 1),
    )


def phase_table(xcoord, nx_total, momenta, source):
    plane_index = jnp.arange(NY * NZ, dtype=jnp.int32)
    ycoord = plane_index // NZ
    zcoord = plane_index % NZ
    dist_x = jnp.mod(xcoord - source[0], nx_total)
    dist_y = jnp.mod(ycoord - source[1], NY)
    dist_z = jnp.mod(zcoord - source[2], NZ)
    frac_x = jnp.mod(momenta[:, 0:1] * dist_x[None, :], nx_total).astype(jnp.float32) / float(
        nx_total
    )
    frac_y = jnp.mod(momenta[:, 1:2] * dist_y[None, :], NY).astype(jnp.float32) / float(NY)
    frac_z = jnp.mod(momenta[:, 2:3] * dist_z[None, :], NZ).astype(jnp.float32) / float(NZ)
    frac = frac_x[:, :, None] + frac_y[:, None, :] + frac_z[:, None, :]
    angle = 2.0 * math.pi * frac
    return jnp.concatenate([jnp.cos(angle), -jnp.sin(angle)], axis=0)


def of_everyone(shard, axis):
    size = lax.axis_size(axis)
    total = shard
    for distance in range(1, size):
        total = total + passed_along(shard, axis, distance)
    return total


def body(sink, links, section_index, momenta, source):
    every = sink.shape[0]
    space_cells = sink.shape[5]
    whole_field = sink.reshape(every * TILES, 8, 128)
    links = links.reshape(links.shape[0], 72, 8, 128)
    index = section_index[::-1, ::-1].reshape(-1)
    laps = index.shape[0]

    starts = [sum(CHUNKS[:i]) for i in range(len(CHUNKS))]
    state = []
    for start, columns in zip(starts, CHUNKS):
        raw = whole_field[start * TILES : (start + columns) * TILES]
        pulled, low, high = first_messages(index, links, whole_field, start, columns)
        field = (whole_field, start)
        state.append((field, field, exchanged(raw, pulled, low, high)))
    buffer = None
    densities = []
    for lap in range(laps):
        for chunk, (start, columns) in enumerate(zip(starts, CHUNKS)):
            centre, aux, arrived = state[chunk]
            if lap == laps - 1:
                buffer, density = lap_call(
                    lap, index, links, centre, arrived, aux, columns, (start, every, buffer)
                )
                densities.append(density)
                continue
            made = lap_call(lap, index, links, centre, arrived, aux, columns)
            field = made[0]
            if lap % 3 == 1:
                aux = (made[1], 0)
            elif lap % 3 == 2:
                aux = (field, 0)
            state[chunk] = ((field, 0), aux, exchanged(field, *made[-3:]))

    density = sum(densities)
    nx_total = space_cells * lax.axis_size("xyz")
    xcoord = lax.axis_index("xyz") * space_cells + jnp.arange(space_cells, dtype=jnp.int32)
    table = phase_table(xcoord, nx_total, momenta, source)
    projected = jnp.sum(table * density[None], axis=(1, 2))
    scale = 1.0 / math.sqrt(576.0 * nx_total * NY * NZ)
    projected = of_everyone(projected * scale, "xyz")
    return (buffer.reshape(sink.shape), projected.reshape(2, momenta.shape[0], 1))


def solution(mesh):
    in_specs = (
        P("cfg", None, None, None, "ta", "xyz", None),
        P("cfg", None, None, None, None, "ta", "xyz", None),
        P(),
        P(),
        P(),
    )
    out_specs = (P("cfg", None, None, None, "ta", "xyz", None), P("cfg", None, "ta"))
    return jax.shard_map(body, mesh=mesh, in_specs=in_specs, out_specs=out_specs, check_vma=False)
```

```python
import functools
import math

import jax
import jax.numpy as jnp
from jax import lax
from jax.experimental import pallas as pl
from jax.experimental.pallas import tpu as pltpu
from jax.sharding import PartitionSpec as P

STEPS = 2
NY = 16
NZ = 8
TILES = 24
CHUNKS = (6, 6)
PAD = 40
VMEM_LIMIT = 16 * 1024 * 1024


flow_step = 0.05
coef_third = 0.75 * flow_step
coef_second = 8.0 * flow_step / 9.0
coef_first = 0.25 * flow_step
coef_mixed = 2.0 * flow_step / 9.0


def link_tile(ref, direction, row, column):
    at = ((direction * 3 + row) * 3 + column) * 2
    return ref[0, at], ref[0, at + 1]


def forward(ref, direction, vector):
    out = []
    for row in range(3):
        real = imag = None
        for column in range(3):
            wr, wi = link_tile(ref, direction, row, column)
            vr, vi = vector[column]
            re = wr * vr - wi * vi
            im = wr * vi + wi * vr
            real = re if real is None else real + re
            imag = im if imag is None else imag + im
        out.append((real, imag))
    return out


def backward(ref, direction, vector):
    out = []
    for row in range(3):
        real = imag = None
        for column in range(3):
            wr, wi = link_tile(ref, direction, column, row)
            vr, vi = vector[column]
            re = wr * vr + wi * vi
            im = wr * vi - wi * vr
            real = re if real is None else real + re
            imag = im if imag is None else imag + im
        out.append((real, imag))
    return out


def each(function, *vectors):
    return [
        tuple(function(*(vector[colour][part] for vector in vectors)) for part in range(2))
        for colour in range(3)
    ]


def tiles_of(ref, base):
    return [(ref[base + 2 * colour], ref[base + 2 * colour + 1]) for colour in range(3)]


def rows_of(ref, base):
    return [
        tuple(
            jnp.broadcast_to(ref[pl.ds(base + 2 * colour + part, 1), :], (8, 128))
            for part in range(2)
        )
        for colour in range(3)
    ]


def put_tiles(ref, base, vector):
    for colour in range(3):
        for part in range(2):
            ref[base + 2 * colour + part] = vector[colour][part]


def put_rows(ref, base, vector, row):
    for colour in range(3):
        for part in range(2):
            ref[pl.ds(base + 2 * colour + part, 1), :] = vector[colour][part][row : row + 1, :]


def roll(value, shift, axis):
    return pltpu.roll(value, shift % value.shape[axis], axis)


def messages(next_ref, base, field, pulled_ref, low_ref, high_ref):
    put_tiles(pulled_ref, base, backward(next_ref, 0, field))
    put_rows(low_ref, base, field, 0)
    put_rows(high_ref, base, backward(next_ref, 1, field), 7)


def first_kernel(
    start, columns, index_ref, field_ref, links_ref, raw_ref, pulled_ref, low_ref, high_ref, next_ref, sems
):
    field_copy = pltpu.make_async_copy(
        field_ref.at[pl.ds(start * TILES, columns * TILES)], raw_ref, sems.at[0]
    )
    link_copy = pltpu.make_async_copy(
        links_ref.at[pl.ds(slot_of(index_ref, 0), 1), pl.ds(0, 36)], next_ref, sems.at[1]
    )
    field_copy.start()
    link_copy.start()
    field_copy.wait()
    link_copy.wait()

    @pl.loop(0, columns)
    def _(column):
        for spin in range(4):
            base = pl.multiple_of(column * TILES, TILES) + 6 * spin
            messages(next_ref, base, tiles_of(raw_ref, base), pulled_ref, low_ref, high_ref)


def local_terms(spin, centre, centre_ref, right_ref, left_ref, link_ref, masks, total):
    base = 6 * spin
    is_top, is_bottom, is_far, is_near = masks
    add = functools.partial(each, lambda a, b: a + b)
    above_x = each(
        lambda v, h: jnp.where(is_top, h, roll(v, -1, 0)), centre, rows_of(right_ref, base)
    )
    total = add(total, forward(link_ref, 1, above_x))
    below_x = each(
        lambda v, h: jnp.where(is_bottom, h, roll(v, 1, 0)),
        backward(link_ref, 1, centre),
        rows_of(left_ref, base),
    )
    total = add(total, below_x)
    total = add(total, forward(link_ref, 2, each(lambda v: roll(v, -NZ, 1), centre)))
    total = add(total, each(lambda v: roll(v, NZ, 1), backward(link_ref, 2, centre)))
    above_z = each(lambda v: jnp.where(is_far, roll(v, NZ - 1, 1), roll(v, -1, 1)), centre)
    total = add(total, forward(link_ref, 3, above_z))
    below_z = each(
        lambda v: jnp.where(is_near, roll(v, 1 - NZ, 1), roll(v, 1, 1)),
        backward(link_ref, 3, centre),
    )
    return add(total, below_z)


def edge_masks():
    sub = lax.broadcasted_iota(jnp.int32, (8, 128), 0)
    zcoord = lax.broadcasted_iota(jnp.int32, (8, 128), 1) % NZ
    return sub == 7, sub == 0, zcoord == NZ - 1, zcoord == 0


def lap_kernel(kind, index_ref, *refs):
    refs = list(refs)
    centre_ref, above_ref, below_ref, right_ref, left_ref, link_ref = refs[:6]
    refs = refs[6:]
    aux_ref = refs.pop(0) if kind > 0 else None
    next_ref, out_ref = refs[:2]
    refs = refs[2:]
    sum_ref = refs.pop(0) if kind == 1 else None
    pulled_ref, low_ref, high_ref = refs

    masks = edge_masks()
    add = functools.partial(each, lambda a, b: a + b)
    for spin in range(4):
        base = 6 * spin
        centre = tiles_of(centre_ref, base)
        total = each(lambda v, p: p - 8.0 * v, centre, tiles_of(below_ref, base))
        total = add(total, forward(link_ref, 0, tiles_of(above_ref, base)))
        total = local_terms(spin, centre, centre_ref, right_ref, left_ref, link_ref, masks, total)
        if kind == 0:
            field = each(lambda t: coef_third * t, total)
        elif kind == 1:
            middle = each(lambda a, t: a + coef_second * t, tiles_of(aux_ref, base), total)
            field = each(lambda m, v: coef_first * m - coef_mixed * v, middle, centre)
            put_tiles(sum_ref, base, add(middle, centre))
        else:
            field = add(tiles_of(aux_ref, base), total)
        put_tiles(out_ref, base, field)
        messages(next_ref, base, field, pulled_ref, low_ref, high_ref)


def local_kernel(index_ref, centre_ref, right_ref, left_ref, link_ref, aux_ref, out_ref):
    masks = edge_masks()
    for spin in range(4):
        base = 6 * spin
        centre = tiles_of(centre_ref, base)
        total = each(lambda v, a: a - 8.0 * v, centre, tiles_of(aux_ref, base))
        total = local_terms(spin, centre, centre_ref, right_ref, left_ref, link_ref, masks, total)
        put_tiles(out_ref, base, total)


def final_kernel(last, scale, index_ref, *refs):
    refs = list(refs)
    partial_ref, above_ref, below_ref, link_ref = refs[:4]
    if last:
        before_ref, table_ref = refs[4:6]
    out_ref, result_ref = refs[-3:-1] if last else refs[-2:]
    total_ref = refs[-1] if last else result_ref
    density = None
    for spin in range(4):
        base = 6 * spin
        total = each(lambda a, b: a + b, tiles_of(partial_ref, base), tiles_of(below_ref, base))
        field = each(
            lambda a, b: a + b, total, forward(link_ref, 0, tiles_of(above_ref, base))
        )
        put_tiles(out_ref, base, field)
        part = None
        for colour in range(3):
            for value in field[colour]:
                part = value * value if part is None else part + value * value
        if density is None:
            density = part
        elif spin < 2:
            density = density + part
        else:
            density = density - part

    @pl.when(pl.program_id(0) == 0)
    def _():
        total_ref[...] = density + before_ref[...] if last else density

    @pl.when(pl.program_id(0) > 0)
    def _():
        total_ref[...] = total_ref[...] + density

    if last:

        @pl.when(pl.program_id(0) == pl.num_programs(0) - 1)
        def _():
            sums = None
            for row in range(8):
                whole = jnp.broadcast_to(total_ref[row : row + 1, :], table_ref.shape[1:])
                term = table_ref[row] * whole
                sums = term if sums is None else sums + term
            ones = jnp.full((8, 128), scale, jnp.float32)
            answer = lax.dot_general(
                ones,
                sums,
                (((1,), (1,)), ((), ())),
                precision=lax.Precision.HIGHEST,
                preferred_element_type=jnp.float32,
            )
            for row in range(result_ref.shape[0]):
                result_ref[row] = answer[0:1, :]


def phase_kernel(nx_total, source_ref, momenta_ref, after_ref, table_ref):
    count = momenta_ref.shape[0]
    lanes = lax.broadcasted_iota(jnp.int32, (count, 128), 1)

    def within(value, size):
        return jnp.bitwise_and(value, size - 1)

    def fraction(axis, distance, size):
        momentum = jnp.broadcast_to(momenta_ref[:, axis : axis + 1], (count, 128))
        return within(momentum * within(distance, size), size).astype(jnp.float32) * (1.0 / size)

    rest = fraction(1, lanes // NZ - source_ref[1], NY)
    rest_z = fraction(2, lanes % NZ - source_ref[2], NZ)
    table_ref[...] = jnp.zeros(table_ref.shape, jnp.float32)
    first = lax.axis_index("xyz") * 8

    @pl.loop(0, 8)
    def _(row):
        xcoord = jnp.full((count, 128), first + row - source_ref[0], jnp.int32)
        angle = 2.0 * math.pi * (fraction(0, xcoord, nx_total) + rest + rest_z)
        table_ref[row, 0:count, :] = jnp.cos(angle)
        table_ref[row, PAD : PAD + count, :] = -jnp.sin(angle)


def total_kernel(all_ref, out_ref):
    count = out_ref.shape[2]
    total = jnp.sum(all_ref[...], axis=0)
    out_ref[0] = total[:, 0:count]
    out_ref[1] = total[:, PAD : PAD + count]


def field_spec(offset):
    return pl.BlockSpec((TILES, 8, 128), lambda i, index: (i + offset, 0, 0))


def rows_spec():
    return pl.BlockSpec((TILES, 128), lambda i, index: (i, 0))


def slot_of(index, lap):
    return index[STEPS - 1 - lap // 3, 2 - lap % 3]


def links_spec(lap, tiles):
    return pl.BlockSpec((1, tiles, 8, 128), lambda i, index: (slot_of(index, lap), 0, 0, 0))


def shape(*dims):
    return jax.ShapeDtypeStruct(dims, jnp.float32)


def cost(columns, per_spin, arrays):
    return pl.CostEstimate(
        flops=columns * 4 * per_spin * 1024,
        bytes_accessed=columns * TILES * 4096 * arrays,
        transcendentals=0,
    )


def params():
    return pltpu.CompilerParams(vmem_limit_bytes=VMEM_LIMIT)


def whole_spec():
    return pl.BlockSpec(memory_space=pltpu.VMEM)


def first_messages(index, links, field, start, columns):
    hbm = pl.BlockSpec(memory_space=pltpu.HBM)
    return pl.pallas_call(
        functools.partial(first_kernel, start, columns),
        grid_spec=pltpu.PrefetchScalarGridSpec(
            num_scalar_prefetch=1,
            grid=(),
            in_specs=[hbm, hbm],
            out_specs=[whole_spec()] * 4,
            scratch_shapes=[
                pltpu.VMEM((1, 36, 8, 128), jnp.float32),
                pltpu.SemaphoreType.DMA((2,)),
            ],
        ),
        out_shape=[shape(columns * TILES, 8, 128)] * 2 + [shape(columns * TILES, 128)] * 2,
        compiler_params=params(),
        cost_estimate=cost(columns, 140, 2),
        name="first_messages",
    )(index, field, links)


def lap_call(lap, index, links, centre, arrived, aux, columns):
    kind = lap % 3
    above, below, right, left = arrived
    operands = [centre, above, below, right, left, links]
    in_specs = [field_spec(0)] * 3 + [rows_spec()] * 2 + [links_spec(lap, 72)]
    if kind > 0:
        operands.append(aux)
        in_specs.append(field_spec(0))
    operands.append(links)
    in_specs.append(links_spec(lap + 1, 36))
    fields = 3 if kind == 1 else 2
    return pl.pallas_call(
        functools.partial(lap_kernel, kind),
        grid_spec=pltpu.PrefetchScalarGridSpec(
            num_scalar_prefetch=1,
            grid=(columns,),
            in_specs=in_specs,
            out_specs=[field_spec(0)] * fields + [rows_spec()] * 2,
        ),
        out_shape=[shape(columns * TILES, 8, 128)] * fields + [shape(columns * TILES, 128)] * 2,
        compiler_params=params(),
        cost_estimate=cost(columns, 700, 6),
        name=f"lap{lap}_{columns}",
    )(index, *operands)


def local_call(lap, index, links, centre, right, left, aux, columns):
    return pl.pallas_call(
        local_kernel,
        grid_spec=pltpu.PrefetchScalarGridSpec(
            num_scalar_prefetch=1,
            grid=(columns,),
            in_specs=[field_spec(0), rows_spec(), rows_spec(), links_spec(lap, 72), field_spec(0)],
            out_specs=field_spec(0),
        ),
        out_shape=shape(columns * TILES, 8, 128),
        compiler_params=params(),
        cost_estimate=cost(columns, 450, 3),
        name=f"local{lap}_{columns}",
    )(index, centre, right, left, links, aux)


def final_call(lap, index, links, partial, above, below, start, columns, every, buffer, more, scale):
    last = more is not None
    operands = [partial, above, below, links]
    in_specs = [field_spec(0)] * 3 + [links_spec(lap, 18)]
    result_spec = pl.BlockSpec((8, 128), lambda i, index: (0, 0))
    result_shape = shape(8, 128)
    scratch = []
    if last:
        before, table, size = more
        operands += [before, table]
        in_specs += [whole_spec()] * 2
        result_spec = pl.BlockSpec((size, 1, table.shape[1]), lambda i, index: (0, 0, 0))
        result_shape = shape(size, 1, table.shape[1])
        scratch = [pltpu.VMEM((8, 128), jnp.float32)]
    aliases = {}
    if buffer is not None:
        aliases = {len(operands) + 1: 0}
        operands.append(buffer)
        in_specs.append(pl.BlockSpec(memory_space=pl.ANY))
    return pl.pallas_call(
        functools.partial(final_kernel, last, scale),
        grid_spec=pltpu.PrefetchScalarGridSpec(
            num_scalar_prefetch=1,
            grid=(columns,),
            in_specs=in_specs,
            out_specs=[field_spec(start), result_spec],
            scratch_shapes=scratch,
        ),
        out_shape=[shape(every * TILES, 8, 128), result_shape],
        input_output_aliases=aliases,
        compiler_params=params(),
        cost_estimate=cost(columns, 100, 4),
        name=f"final{start}_{columns}",
    )(index, *operands)


def phase_call(nx_total, momenta, source, after):
    smem = pl.BlockSpec(memory_space=pltpu.SMEM)
    return pl.pallas_call(
        functools.partial(phase_kernel, nx_total),
        in_specs=[smem, whole_spec(), pl.BlockSpec(memory_space=pl.ANY)],
        out_specs=whole_spec(),
        out_shape=shape(8, 2 * PAD, 128),
        compiler_params=params(),
        cost_estimate=pl.CostEstimate(flops=8_000_000, bytes_accessed=400_000, transcendentals=0),
        name="phases",
    )(source, momenta, after)


def total_call(everything, count):
    return pl.pallas_call(
        total_kernel,
        in_specs=[whole_spec()],
        out_specs=whole_spec(),
        out_shape=shape(2, 1, count),
        compiler_params=params(),
        cost_estimate=pl.CostEstimate(flops=10_000, bytes_accessed=10_000, transcendentals=0),
        name="total",
    )(everything)


def passed_along(block, axis, distance):
    devices = range(lax.axis_size(axis))
    route = [((i - distance) % len(devices), i) for i in devices]
    return lax.ppermute(block, axis, route)


def exchanged(field, pulled, low, high):
    return (
        passed_along(field, "ta", -1),
        passed_along(pulled, "ta", 1),
        passed_along(low, "xyz", -1),
        passed_along(high, "xyz", 1),
    )


def body(sink, links, section_index, momenta, source):
    every = sink.shape[0]
    size = lax.axis_size("xyz")
    nx_total = sink.shape[5] * size
    whole_field = sink.reshape(every * TILES, 8, 128)
    links = links.reshape(links.shape[0], 72, 8, 128)
    laps = 3 * STEPS

    starts = [sum(CHUNKS[:i]) for i in range(len(CHUNKS))]
    state = []
    for start, columns in zip(starts, CHUNKS):
        raw, *made = first_messages(section_index, links, whole_field, start, columns)
        state.append((raw, raw, exchanged(raw, *made)))
    table = None
    for lap in range(laps - 1):
        for chunk, columns in enumerate(CHUNKS):
            centre, aux, arrived = state[chunk]
            made = lap_call(lap, section_index, links, centre, arrived, aux, columns)
            field = made[0]
            if lap % 3 == 1:
                aux = made[1]
            elif lap % 3 == 2:
                aux = field
            state[chunk] = (field, aux, exchanged(field, *made[-3:]))
        if lap == 1:
            table = phase_call(nx_total, momenta, source, made[-1])

    scale = 1.0 / math.sqrt(576.0 * nx_total * NY * NZ)
    buffer = density = None
    for chunk, (start, columns) in enumerate(zip(starts, CHUNKS)):
        centre, aux, (above, below, right, left) = state[chunk]
        lap = laps - 1
        partial = local_call(lap, section_index, links, centre, right, left, aux, columns)
        more = (density, table, size) if chunk == len(CHUNKS) - 1 else None
        buffer, result = final_call(
            lap, section_index, links, partial, above, below, start, columns, every, buffer, more, scale
        )
        density = result if density is None else density + result if more is None else result
    everything = lax.all_to_all(density, "xyz", split_axis=0, concat_axis=0, tiled=True)
    correlator = total_call(everything, momenta.shape[0])
    return (buffer.reshape(sink.shape), correlator.reshape(2, momenta.shape[0], 1))


def solution(mesh):
    in_specs = (
        P("cfg", None, None, None, "ta", "xyz", None),
        P("cfg", None, None, None, None, "ta", "xyz", None),
        P(),
        P(),
        P(),
    )
    out_specs = (P("cfg", None, None, None, "ta", "xyz", None), P("cfg", None, "ta"))
    return jax.shard_map(body, mesh=mesh, in_specs=in_specs, out_specs=out_specs, check_vma=False)
```

```python
import functools
import math

import jax
import jax.numpy as jnp
from jax import lax
from jax.experimental import pallas as pl
from jax.experimental.pallas import tpu as pltpu
from jax.sharding import PartitionSpec as P

STEPS = 2
NY = 16
NZ = 8
TILES = 24
CHUNKS = (6, 6)
PAD = 64
VMEM_LIMIT = 16 * 1024 * 1024


flow_step = 0.05
coef_third = 0.75 * flow_step
coef_second = 8.0 * flow_step / 9.0
coef_first = 0.25 * flow_step
coef_mixed = 2.0 * flow_step / 9.0


def link_tile(links, direction, row, column):
    ref, slot = links
    at = ((direction * 3 + row) * 3 + column) * 2
    return ref[slot, at], ref[slot, at + 1]


def forward(links, direction, vector):
    out = []
    for row in range(3):
        real = imag = None
        for column in range(3):
            wr, wi = link_tile(links, direction, row, column)
            vr, vi = vector[column]
            re = wr * vr - wi * vi
            im = wr * vi + wi * vr
            real = re if real is None else real + re
            imag = im if imag is None else imag + im
        out.append((real, imag))
    return out


def backward(links, direction, vector):
    out = []
    for row in range(3):
        real = imag = None
        for column in range(3):
            wr, wi = link_tile(links, direction, column, row)
            vr, vi = vector[column]
            re = wr * vr + wi * vi
            im = wr * vi - wi * vr
            real = re if real is None else real + re
            imag = im if imag is None else imag + im
        out.append((real, imag))
    return out


def each(function, *vectors):
    return [
        tuple(function(*(vector[colour][part] for vector in vectors)) for part in range(2))
        for colour in range(3)
    ]


def tiles_of(ref, base):
    return [(ref[base + 2 * colour], ref[base + 2 * colour + 1]) for colour in range(3)]


def rows_of(ref, base):
    return [
        tuple(
            jnp.broadcast_to(ref[pl.ds(base + 2 * colour + part, 1), :], (8, 128))
            for part in range(2)
        )
        for colour in range(3)
    ]


def put_tiles(ref, base, vector):
    for colour in range(3):
        for part in range(2):
            ref[base + 2 * colour + part] = vector[colour][part]


def put_rows(ref, base, vector, row):
    for colour in range(3):
        for part in range(2):
            ref[pl.ds(base + 2 * colour + part, 1), :] = vector[colour][part][row : row + 1, :]


def roll(value, shift, axis):
    return pltpu.roll(value, shift % value.shape[axis], axis)


def messages(links, base, field, pulled_ref, low_ref, high_ref):
    put_tiles(pulled_ref, base, backward(links, 0, field))
    put_rows(low_ref, base, field, 0)
    put_rows(high_ref, base, backward(links, 1, field), 7)


def each_vector(columns):
    def loop(work):
        @pl.loop(0, columns)
        def _(column):
            for spin in range(4):
                work(spin, pl.multiple_of(column * TILES, TILES) + 6 * spin)

    return loop


def first_kernel(
    start, columns, index_ref, field_ref, links_ref, raw_ref, pulled_ref, low_ref, high_ref, next_ref, sems
):
    field_copy = pltpu.make_async_copy(
        field_ref.at[pl.ds(start * TILES, columns * TILES)], raw_ref, sems.at[0]
    )
    link_copy = pltpu.make_async_copy(
        links_ref.at[pl.ds(slot_of(index_ref, 0), 1), pl.ds(0, 36)], next_ref, sems.at[1]
    )
    field_copy.start()
    link_copy.start()
    field_copy.wait()
    link_copy.wait()

    @each_vector(columns)
    def _(spin, base):
        messages((next_ref, 0), base, tiles_of(raw_ref, base), pulled_ref, low_ref, high_ref)


def local_terms(base, centre, right_ref, left_ref, links, masks, total):
    is_top, is_bottom, is_far, is_near = masks
    add = functools.partial(each, lambda a, b: a + b)
    above_x = each(
        lambda v, h: jnp.where(is_top, h, roll(v, -1, 0)), centre, rows_of(right_ref, base)
    )
    total = add(total, forward(links, 1, above_x))
    below_x = each(
        lambda v, h: jnp.where(is_bottom, h, roll(v, 1, 0)),
        backward(links, 1, centre),
        rows_of(left_ref, base),
    )
    total = add(total, below_x)
    total = add(total, forward(links, 2, each(lambda v: roll(v, -NZ, 1), centre)))
    total = add(total, each(lambda v: roll(v, NZ, 1), backward(links, 2, centre)))
    above_z = each(lambda v: jnp.where(is_far, roll(v, NZ - 1, 1), roll(v, -1, 1)), centre)
    total = add(total, forward(links, 3, above_z))
    below_z = each(
        lambda v: jnp.where(is_near, roll(v, 1 - NZ, 1), roll(v, 1, 1)),
        backward(links, 3, centre),
    )
    return add(total, below_z)


def edge_masks():
    sub = lax.broadcasted_iota(jnp.int32, (8, 128), 0)
    zcoord = lax.broadcasted_iota(jnp.int32, (8, 128), 1) % NZ
    return sub == 7, sub == 0, zcoord == NZ - 1, zcoord == 0


def lap_kernel(lap, columns, nx_total, index_ref, *refs):
    kind = lap % 3
    refs = list(refs)
    centre_ref, above_ref, below_ref, right_ref, left_ref, links_ref = refs[:6]
    refs = refs[6:]
    aux_ref = refs.pop(0) if kind > 0 else None
    if nx_total:
        source_ref, momenta_ref = refs[:2]
        refs = refs[2:]
        both_ref = refs.pop()
        phases(nx_total, source_ref, momenta_ref, refs.pop(), both_ref)
    out_ref = refs.pop(0)
    sum_ref = refs.pop(0) if kind == 1 else None
    pulled_ref, low_ref, high_ref = refs

    links = (links_ref, slot_of(index_ref, lap))
    links_next = (links_ref, slot_of(index_ref, lap + 1))
    masks = edge_masks()
    add = functools.partial(each, lambda a, b: a + b)

    @each_vector(columns)
    def _(spin, base):
        centre = tiles_of(centre_ref, base)
        total = each(lambda v, p: p - 8.0 * v, centre, tiles_of(below_ref, base))
        total = add(total, forward(links, 0, tiles_of(above_ref, base)))
        total = local_terms(base, centre, right_ref, left_ref, links, masks, total)
        if kind == 0:
            field = each(lambda t: coef_third * t, total)
        elif kind == 1:
            middle = each(lambda a, t: a + coef_second * t, tiles_of(aux_ref, base), total)
            field = each(lambda m, v: coef_first * m - coef_mixed * v, middle, centre)
            put_tiles(sum_ref, base, add(middle, centre))
        else:
            field = add(tiles_of(aux_ref, base), total)
        put_tiles(out_ref, base, field)
        messages(links_next, base, field, pulled_ref, low_ref, high_ref)


def local_kernel(
    lap, columns, index_ref, centre_ref, right_ref, left_ref, links_ref, aux_ref, out_ref
):
    links = (links_ref, slot_of(index_ref, lap))
    masks = edge_masks()

    @each_vector(columns)
    def _(spin, base):
        centre = tiles_of(centre_ref, base)
        total = each(lambda v, a: a - 8.0 * v, centre, tiles_of(aux_ref, base))
        total = local_terms(base, centre, right_ref, left_ref, links, masks, total)
        put_tiles(out_ref, base, total)


def final_kernel(lap, start, columns, last, scale, index_ref, *refs):
    refs = list(refs)
    partial_ref, above_ref, below_ref, links_ref, before_ref = refs[:5]
    table_ref = refs[5] if last else None
    out_ref, result_ref, held_ref, total_ref, sems = refs[-5:]
    links = (links_ref, slot_of(index_ref, lap))
    total_ref[...] = before_ref[...] if start else jnp.zeros((8, 128), jnp.float32)

    def copy_out(column):
        return pltpu.make_async_copy(
            held_ref.at[pl.ds(column * TILES, TILES)],
            out_ref.at[pl.ds((start + column) * TILES, TILES)],
            sems.at[column],
        )

    @pl.loop(0, columns)
    def _(column):
        density = total_ref[...]
        for spin in range(4):
            base = pl.multiple_of(column * TILES, TILES) + 6 * spin
            total = each(lambda a, b: a + b, tiles_of(partial_ref, base), tiles_of(below_ref, base))
            field = each(
                lambda a, b: a + b, total, forward(links, 0, tiles_of(above_ref, base))
            )
            put_tiles(held_ref, base, field)
            part = None
            for colour in range(3):
                for value in field[colour]:
                    part = value * value if part is None else part + value * value
            density = density + part if spin < 2 else density - part
        total_ref[...] = density
        copy_out(column).start()

    if last:
        sums = None
        for row in range(8):
            phase = table_ref[pl.ds(row * 128, 128), :]
            term = lax.dot_general(
                jnp.broadcast_to(total_ref[row : row + 1, :] * scale, (8, 128)),
                phase,
                (((1,), (0,)), ((), ())),
                precision=lax.Precision.HIGHEST,
                preferred_element_type=jnp.float32,
            )
            sums = term if sums is None else sums + term
        for row in range(result_ref.shape[0]):
            result_ref[row] = sums[0:1, :]
    else:
        result_ref[...] = total_ref[...]

    @pl.loop(0, columns)
    def _(column):
        copy_out(column).wait()


def phases(nx_total, source_ref, momenta_ref, table_ref, both_ref):
    count = momenta_ref.shape[1]
    both_ref[...] = jnp.zeros(both_ref.shape, jnp.int32)
    both_ref[0:3, 0:count] = momenta_ref[...]
    both = both_ref[...]
    both_ref[...] = both + roll(both, PAD, 1)
    sites = lax.broadcasted_iota(jnp.int32, (128, 128), 0)
    quarter = jnp.where(lax.broadcasted_iota(jnp.int32, (128, 128), 1) >= PAD, 0.25, 0.0)

    def within(value, size):
        return jnp.bitwise_and(value, size - 1)

    def fraction(axis, distance, size):
        momentum = jnp.broadcast_to(both_ref[axis : axis + 1, :], (128, 128))
        return within(momentum * within(distance, size), size).astype(jnp.float32) * (1.0 / size)

    plane = fraction(1, sites // NZ - source_ref[1], NY) + quarter
    plane = plane + fraction(2, within(sites, NZ) - source_ref[2], NZ)
    first = lax.axis_index("xyz") * 8

    @pl.loop(0, 8)
    def _(row):
        xcoord = jnp.full((128, 128), first + row - source_ref[0], jnp.int32)
        turns = plane + fraction(0, xcoord, nx_total)
        turns = turns - jnp.floor(turns)
        table_ref[pl.ds(pl.multiple_of(row * 128, 128), 128), :] = jnp.cos(2.0 * math.pi * turns)


def total_kernel(all_ref, out_ref):
    count = out_ref.shape[2]
    total = jnp.sum(all_ref[...], axis=0)
    out_ref[0] = total[:, 0:count]
    out_ref[1] = total[:, PAD : PAD + count]


def slot_of(index, lap):
    return index[STEPS - 1 - lap // 3, 2 - lap % 3]


def shape(*dims):
    return jax.ShapeDtypeStruct(dims, jnp.float32)


def cost(columns, per_spin, arrays):
    return pl.CostEstimate(
        flops=columns * 4 * per_spin * 1024,
        bytes_accessed=columns * TILES * 4096 * arrays,
        transcendentals=0,
    )


def params():
    return pltpu.CompilerParams(vmem_limit_bytes=VMEM_LIMIT)


def whole_spec():
    return pl.BlockSpec(memory_space=pltpu.VMEM)


SMEM = pl.BlockSpec(memory_space=pltpu.SMEM)
VMEM = pl.BlockSpec(memory_space=pltpu.VMEM)
ANY = pl.BlockSpec(memory_space=pl.ANY)


def first_messages(index, links, field, start, columns):
    return pl.pallas_call(
        functools.partial(first_kernel, start, columns),
        in_specs=[SMEM, ANY, ANY],
        out_specs=[VMEM] * 4,
        scratch_shapes=[
            pltpu.VMEM((1, 36, 8, 128), jnp.float32),
            pltpu.SemaphoreType.DMA((2,)),
        ],
        out_shape=[shape(columns * TILES, 8, 128)] * 2 + [shape(columns * TILES, 128)] * 2,
        compiler_params=params(),
        cost_estimate=cost(columns, 140, 2),
        name="first_messages",
    )(
        index,
        pltpu.with_memory_space_constraint(field, pltpu.HBM),
        pltpu.with_memory_space_constraint(links, pltpu.HBM),
    )


def lap_call(lap, index, links, centre, arrived, aux, columns, phase=None):
    kind = lap % 3
    operands = [index, centre, *arrived, links]
    if kind > 0:
        operands.append(aux)
    in_specs = [SMEM] + [VMEM] * (len(operands) - 1)
    fields = 3 if kind == 1 else 2
    out_shape = [shape(columns * TILES, 8, 128)] * fields + [shape(columns * TILES, 128)] * 2
    scratch, nx_total = [], 0
    if phase is not None:
        nx_total, source, momenta = phase
        operands += [source, momenta.T]
        in_specs += [SMEM, VMEM]
        out_shape.append(shape(8 * 128, 128))
        scratch = [pltpu.VMEM((8, 128), jnp.int32)]
    return pl.pallas_call(
        functools.partial(lap_kernel, lap, columns, nx_total),
        in_specs=in_specs,
        out_specs=[VMEM] * len(out_shape),
        scratch_shapes=scratch,
        out_shape=out_shape,
        compiler_params=params(),
        cost_estimate=cost(columns, 700, 6),
        name=f"lap{lap}_{columns}",
    )(*operands)


def local_call(lap, index, links, centre, right, left, aux, columns):
    return pl.pallas_call(
        functools.partial(local_kernel, lap, columns),
        in_specs=[SMEM] + [VMEM] * 5,
        out_specs=VMEM,
        out_shape=shape(columns * TILES, 8, 128),
        compiler_params=params(),
        cost_estimate=cost(columns, 450, 3),
        name=f"local{lap}_{columns}",
    )(index, centre, right, left, links, aux)


def final_call(lap, index, links, partial, above, below, before, table, start, columns, sizes, scale):
    every, told = sizes
    last = table is not None
    buffer, density = before
    operands = [index, partial, above, below, links, density]
    in_specs = [SMEM] + [VMEM] * 5
    if last:
        operands.append(table)
        in_specs.append(VMEM)
    aliases = {}
    if buffer is not None:
        aliases = {len(operands): 0}
        operands.append(buffer)
        in_specs.append(ANY)
    return pl.pallas_call(
        functools.partial(final_kernel, lap, start, columns, last, scale),
        in_specs=in_specs,
        out_specs=[ANY, VMEM],
        scratch_shapes=[
            pltpu.VMEM((columns * TILES, 8, 128), jnp.float32),
            pltpu.VMEM((8, 128), jnp.float32),
            pltpu.SemaphoreType.DMA((columns,)),
        ],
        out_shape=[
            shape(every * TILES, 8, 128),
            shape(told, 1, 128) if last else shape(8, 128),
        ],
        input_output_aliases=aliases,
        compiler_params=params(),
        cost_estimate=cost(columns, 100, 4),
        name=f"final{start}_{columns}",
    )(*operands)


def total_call(everything, count):
    return pl.pallas_call(
        total_kernel,
        in_specs=[VMEM],
        out_specs=VMEM,
        out_shape=shape(2, 1, count),
        compiler_params=params(),
        cost_estimate=pl.CostEstimate(flops=10_000, bytes_accessed=10_000, transcendentals=0),
        name="total",
    )(everything)


def passed_along(block, axis, distance):
    devices = range(lax.axis_size(axis))
    route = [((i - distance) % len(devices), i) for i in devices]
    return lax.ppermute(block, axis, route)


def exchanged(field, pulled, low, high):
    return (
        passed_along(field, "ta", -1),
        passed_along(pulled, "ta", 1),
        passed_along(low, "xyz", -1),
        passed_along(high, "xyz", 1),
    )


def body(sink, links, section_index, momenta, source):
    every = sink.shape[0]
    size = lax.axis_size("xyz")
    nx_total = sink.shape[5] * size
    whole_field = sink.reshape(every * TILES, 8, 128)
    links = links.reshape(links.shape[0], 72, 8, 128)
    laps = 3 * STEPS

    starts = [sum(CHUNKS[:i]) for i in range(len(CHUNKS))]
    state = []
    for start, columns in zip(starts, CHUNKS):
        raw, *made = first_messages(section_index, links, whole_field, start, columns)
        state.append((raw, raw, exchanged(raw, *made)))
    table = None
    for lap in range(laps - 1):
        for chunk, columns in enumerate(CHUNKS):
            centre, aux, arrived = state[chunk]
            with_table = lap == 2 and chunk == len(CHUNKS) - 1
            phase = (nx_total, source, momenta) if with_table else None
            made = lap_call(lap, section_index, links, centre, arrived, aux, columns, phase)
            if with_table:
                *made, table = made
            field = made[0]
            if lap % 3 == 1:
                aux = made[1]
            elif lap % 3 == 2:
                aux = field
            state[chunk] = (field, aux, exchanged(field, *made[-3:]))

    scale = 1.0 / math.sqrt(576.0 * nx_total * NY * NZ)
    lap = laps - 1
    buffer, result = None, state[0][2][2]
    for chunk, (start, columns) in enumerate(zip(starts, CHUNKS)):
        centre, aux, (above, below, right, left) = state[chunk]
        partial = local_call(lap, section_index, links, centre, right, left, aux, columns)
        last = chunk == len(CHUNKS) - 1
        buffer, result = final_call(
            lap,
            section_index,
            links,
            partial,
            above,
            below,
            (buffer, result),
            table if last else None,
            start,
            columns,
            (every, size),
            scale,
        )
    everything = lax.all_to_all(result, "xyz", split_axis=0, concat_axis=0, tiled=True)
    correlator = total_call(everything, momenta.shape[0])
    return (buffer.reshape(sink.shape), correlator.reshape(2, momenta.shape[0], 1))


def solution(mesh):
    in_specs = (
        P("cfg", None, None, None, "ta", "xyz", None),
        P("cfg", None, None, None, None, "ta", "xyz", None),
        P(),
        P(),
        P(),
    )
    out_specs = (P("cfg", None, None, None, "ta", "xyz", None), P("cfg", None, "ta"))
    return jax.shard_map(body, mesh=mesh, in_specs=in_specs, out_specs=out_specs, check_vma=False)
```

```python
import functools
import math

import jax
import jax.numpy as jnp
from jax import lax
from jax.experimental import pallas as pl
from jax.experimental.pallas import tpu as pltpu
from jax.sharding import PartitionSpec as P

STEPS = 2
NY = 16
NZ = 8
TILES = 24
CHUNKS = (6, 6)
PAD = 64
VMEM_LIMIT = 16 * 1024 * 1024


flow_step = 0.05
coef_third = 0.75 * flow_step
coef_second = 8.0 * flow_step / 9.0
coef_first = 0.25 * flow_step
coef_mixed = 2.0 * flow_step / 9.0


def link_tile(links, direction, row, column):
    ref, slot = links
    at = ((direction * 3 + row) * 3 + column) * 2
    return ref[slot, at], ref[slot, at + 1]


def forward(links, direction, vector):
    out = []
    for row in range(3):
        real = imag = None
        for column in range(3):
            wr, wi = link_tile(links, direction, row, column)
            vr, vi = vector[column]
            re = wr * vr - wi * vi
            im = wr * vi + wi * vr
            real = re if real is None else real + re
            imag = im if imag is None else imag + im
        out.append((real, imag))
    return out


def backward(links, direction, vector):
    out = []
    for row in range(3):
        real = imag = None
        for column in range(3):
            wr, wi = link_tile(links, direction, column, row)
            vr, vi = vector[column]
            re = wr * vr + wi * vi
            im = wr * vi - wi * vr
            real = re if real is None else real + re
            imag = im if imag is None else imag + im
        out.append((real, imag))
    return out


def each(function, *vectors):
    return [
        tuple(function(*(vector[colour][part] for vector in vectors)) for part in range(2))
        for colour in range(3)
    ]


def tiles_of(ref, base):
    return [(ref[base + 2 * colour], ref[base + 2 * colour + 1]) for colour in range(3)]


def rows_of(ref, base):
    return [
        tuple(
            jnp.broadcast_to(ref[pl.ds(base + 2 * colour + part, 1), :], (8, 128))
            for part in range(2)
        )
        for colour in range(3)
    ]


def put_tiles(ref, base, vector):
    for colour in range(3):
        for part in range(2):
            ref[base + 2 * colour + part] = vector[colour][part]


def put_rows(ref, base, vector, row):
    for colour in range(3):
        for part in range(2):
            ref[pl.ds(base + 2 * colour + part, 1), :] = vector[colour][part][row : row + 1, :]


def roll(value, shift, axis):
    return pltpu.roll(value, shift % value.shape[axis], axis)


def messages(links, base, field, pulled_ref, low_ref, high_ref):
    put_tiles(pulled_ref, base, backward(links, 0, field))
    put_rows(low_ref, base, field, 0)
    put_rows(high_ref, base, backward(links, 1, field), 7)


def each_vector(columns):
    def loop(work):
        @pl.loop(0, columns)
        def _(column):
            for spin in range(4):
                work(spin, pl.multiple_of(column * TILES, TILES) + 6 * spin)

    return loop


def first_kernel(
    start, columns, index_ref, field_ref, links_ref, raw_ref, pulled_ref, slots_ref, next_ref, sems
):
    def copy_in(column):
        return pltpu.make_async_copy(
            field_ref.at[pl.ds((start + column) * TILES, TILES)],
            raw_ref.at[pl.ds(column * TILES, TILES)],
            sems.at[column],
        )

    index_copy = pltpu.make_async_copy(index_ref, slots_ref, sems.at[columns])
    link_copy = pltpu.make_async_copy(
        links_ref.at[:, pl.ds(0, 18)], next_ref, sems.at[columns + 1]
    )
    index_copy.start()
    link_copy.start()
    for column in range(columns):
        copy_in(column).start()
    index_copy.wait()
    link_copy.wait()
    links = (next_ref, slot_of(slots_ref, 0))

    @pl.loop(0, columns)
    def _(column):
        copy_in(column).wait()
        for spin in range(4):
            base = pl.multiple_of(column * TILES, TILES) + 6 * spin
            put_tiles(pulled_ref, base, backward(links, 0, tiles_of(raw_ref, base)))


def first_rows_kernel(sizes, index_ref, links_ref, *refs):
    links = (links_ref, slot_of(index_ref, 0))
    for chunk, columns in enumerate(sizes):
        raw_ref = refs[chunk]
        low_ref, high_ref = refs[len(sizes) + 2 * chunk : len(sizes) + 2 * chunk + 2]

        @each_vector(columns)
        def _(spin, base):
            field = tiles_of(raw_ref, base)
            put_rows(low_ref, base, field, 0)
            put_rows(high_ref, base, backward(links, 1, field), 7)


def local_terms(base, centre, right_ref, left_ref, links, masks, total):
    is_top, is_bottom, is_far, is_near = masks
    add = functools.partial(each, lambda a, b: a + b)
    above_x = each(
        lambda v, h: jnp.where(is_top, h, roll(v, -1, 0)), centre, rows_of(right_ref, base)
    )
    total = add(total, forward(links, 1, above_x))
    below_x = each(
        lambda v, h: jnp.where(is_bottom, h, roll(v, 1, 0)),
        backward(links, 1, centre),
        rows_of(left_ref, base),
    )
    total = add(total, below_x)
    total = add(total, forward(links, 2, each(lambda v: roll(v, -NZ, 1), centre)))
    total = add(total, each(lambda v: roll(v, NZ, 1), backward(links, 2, centre)))
    above_z = each(lambda v: jnp.where(is_far, roll(v, NZ - 1, 1), roll(v, -1, 1)), centre)
    total = add(total, forward(links, 3, above_z))
    below_z = each(
        lambda v: jnp.where(is_near, roll(v, 1 - NZ, 1), roll(v, 1, 1)),
        backward(links, 3, centre),
    )
    return add(total, below_z)


def edge_masks():
    sub = lax.broadcasted_iota(jnp.int32, (8, 128), 0)
    zcoord = lax.broadcasted_iota(jnp.int32, (8, 128), 1) % NZ
    return sub == 7, sub == 0, zcoord == NZ - 1, zcoord == 0


def lap_kernel(lap, columns, nx_total, index_ref, *refs):
    kind = lap % 3
    refs = list(refs)
    centre_ref, above_ref, below_ref, right_ref, left_ref, links_ref = refs[:6]
    refs = refs[6:]
    aux_ref = refs.pop(0) if kind > 0 else None
    if nx_total:
        source_ref, momenta_ref = refs[:2]
        refs = refs[2:]
        both_ref = refs.pop()
        phases(nx_total, source_ref, momenta_ref, refs.pop(), both_ref)
    out_ref = refs.pop(0)
    sum_ref = refs.pop(0) if kind == 1 else None
    pulled_ref, low_ref, high_ref = refs

    links = (links_ref, slot_of(index_ref, lap))
    links_next = (links_ref, slot_of(index_ref, lap + 1))
    masks = edge_masks()
    add = functools.partial(each, lambda a, b: a + b)

    @each_vector(columns)
    def _(spin, base):
        centre = tiles_of(centre_ref, base)
        total = each(lambda v, p: p - 8.0 * v, centre, tiles_of(below_ref, base))
        total = add(total, forward(links, 0, tiles_of(above_ref, base)))
        total = local_terms(base, centre, right_ref, left_ref, links, masks, total)
        if kind == 0:
            field = each(lambda t: coef_third * t, total)
        elif kind == 1:
            middle = each(lambda a, t: a + coef_second * t, tiles_of(aux_ref, base), total)
            field = each(lambda m, v: coef_first * m - coef_mixed * v, middle, centre)
            put_tiles(sum_ref, base, add(middle, centre))
        else:
            field = add(tiles_of(aux_ref, base), total)
        put_tiles(out_ref, base, field)
        messages(links_next, base, field, pulled_ref, low_ref, high_ref)


def local_kernel(
    lap, columns, index_ref, centre_ref, right_ref, left_ref, links_ref, aux_ref, out_ref
):
    links = (links_ref, slot_of(index_ref, lap))
    masks = edge_masks()

    @each_vector(columns)
    def _(spin, base):
        centre = tiles_of(centre_ref, base)
        total = each(lambda v, a: a - 8.0 * v, centre, tiles_of(aux_ref, base))
        total = local_terms(base, centre, right_ref, left_ref, links, masks, total)
        put_tiles(out_ref, base, total)


def final_kernel(lap, start, columns, last, scale, index_ref, *refs):
    refs = list(refs)
    partial_ref, above_ref, below_ref, links_ref, before_ref = refs[:5]
    table_ref = refs[5] if last else None
    out_ref, result_ref, held_ref, total_ref, sems = refs[-5:]
    links = (links_ref, slot_of(index_ref, lap))
    total_ref[...] = before_ref[...] if start else jnp.zeros((8, 128), jnp.float32)

    def copy_out(column):
        return pltpu.make_async_copy(
            held_ref.at[pl.ds(column * TILES, TILES)],
            out_ref.at[pl.ds((start + column) * TILES, TILES)],
            sems.at[column],
        )

    @pl.loop(0, columns)
    def _(column):
        density = total_ref[...]
        for spin in range(4):
            base = pl.multiple_of(column * TILES, TILES) + 6 * spin
            total = each(lambda a, b: a + b, tiles_of(partial_ref, base), tiles_of(below_ref, base))
            field = each(
                lambda a, b: a + b, total, forward(links, 0, tiles_of(above_ref, base))
            )
            put_tiles(held_ref, base, field)
            part = None
            for colour in range(3):
                for value in field[colour]:
                    part = value * value if part is None else part + value * value
            density = density + part if spin < 2 else density - part
        total_ref[...] = density
        copy_out(column).start()

    if last:
        sums = None
        for row in range(8):
            phase = table_ref[pl.ds(row * 128, 128), :]
            term = lax.dot_general(
                jnp.broadcast_to(total_ref[row : row + 1, :] * scale, (8, 128)),
                phase,
                (((1,), (0,)), ((), ())),
                precision=lax.Precision.HIGHEST,
                preferred_element_type=jnp.float32,
            )
            sums = term if sums is None else sums + term
        for row in range(result_ref.shape[0]):
            result_ref[row] = sums[0:1, :]
    else:
        result_ref[...] = total_ref[...]

    @pl.loop(0, columns)
    def _(column):
        copy_out(column).wait()


def phases(nx_total, source_ref, momenta_ref, table_ref, both_ref):
    count = momenta_ref.shape[1]
    both_ref[...] = jnp.zeros(both_ref.shape, jnp.int32)
    both_ref[0:3, 0:count] = momenta_ref[...]
    both = both_ref[...]
    both_ref[...] = both + roll(both, PAD, 1)
    sites = lax.broadcasted_iota(jnp.int32, (128, 128), 0)
    quarter = jnp.where(lax.broadcasted_iota(jnp.int32, (128, 128), 1) >= PAD, 0.25, 0.0)

    def within(value, size):
        return jnp.bitwise_and(value, size - 1)

    def fraction(axis, distance, size):
        momentum = jnp.broadcast_to(both_ref[axis : axis + 1, :], (128, 128))
        return within(momentum * within(distance, size), size).astype(jnp.float32) * (1.0 / size)

    plane = fraction(1, sites // NZ - source_ref[1], NY) + quarter
    plane = plane + fraction(2, within(sites, NZ) - source_ref[2], NZ)
    first = lax.axis_index("xyz") * 8

    @pl.loop(0, 8)
    def _(row):
        xcoord = jnp.full((128, 128), first + row - source_ref[0], jnp.int32)
        turns = plane + fraction(0, xcoord, nx_total)
        turns = turns - jnp.floor(turns)
        table_ref[pl.ds(pl.multiple_of(row * 128, 128), 128), :] = jnp.cos(2.0 * math.pi * turns)


def total_kernel(all_ref, out_ref):
    count = out_ref.shape[2]
    total = jnp.sum(all_ref[...], axis=0)
    out_ref[0] = total[:, 0:count]
    out_ref[1] = total[:, PAD : PAD + count]


def slot_of(index, lap):
    return index[STEPS - 1 - lap // 3, 2 - lap % 3]


def shape(*dims):
    return jax.ShapeDtypeStruct(dims, jnp.float32)


def cost(columns, per_spin, arrays):
    return pl.CostEstimate(
        flops=columns * 4 * per_spin * 1024,
        bytes_accessed=columns * TILES * 4096 * arrays,
        transcendentals=0,
    )


def params():
    return pltpu.CompilerParams(vmem_limit_bytes=VMEM_LIMIT)


def whole_spec():
    return pl.BlockSpec(memory_space=pltpu.VMEM)


SMEM = pl.BlockSpec(memory_space=pltpu.SMEM)
VMEM = pl.BlockSpec(memory_space=pltpu.VMEM)
ANY = pl.BlockSpec(memory_space=pl.ANY)


def first_messages(index, links, field, start, columns):
    return pl.pallas_call(
        functools.partial(first_kernel, start, columns),
        in_specs=[ANY] * 3,
        out_specs=[VMEM] * 2,
        scratch_shapes=[
            pltpu.SMEM(index.shape, jnp.int32),
            pltpu.VMEM((links.shape[0], 18, 8, 128), jnp.float32),
            pltpu.SemaphoreType.DMA((columns + 2,)),
        ],
        out_shape=[shape(columns * TILES, 8, 128)] * 2,
        compiler_params=params(),
        cost_estimate=cost(columns, 70, 2),
        name="first_messages",
    )(*(pltpu.with_memory_space_constraint(a, pltpu.HBM) for a in (index, field, links)))


def first_rows(index, links, fields, sizes):
    shapes = [shape(columns * TILES, 128) for columns in sizes for _ in range(2)]
    return pl.pallas_call(
        functools.partial(first_rows_kernel, sizes),
        in_specs=[SMEM] + [VMEM] * (1 + len(fields)),
        out_specs=[VMEM] * len(shapes),
        out_shape=shapes,
        compiler_params=params(),
        cost_estimate=cost(sum(sizes), 70, 1),
        name="first_rows",
    )(index, links, *fields)


def lap_call(lap, index, links, centre, arrived, aux, columns, phase=None):
    kind = lap % 3
    operands = [index, centre, *arrived, links]
    if kind > 0:
        operands.append(aux)
    in_specs = [SMEM] + [VMEM] * (len(operands) - 1)
    fields = 3 if kind == 1 else 2
    out_shape = [shape(columns * TILES, 8, 128)] * fields + [shape(columns * TILES, 128)] * 2
    scratch, nx_total = [], 0
    if phase is not None:
        nx_total, source, momenta = phase
        operands += [source, momenta.T]
        in_specs += [SMEM, VMEM]
        out_shape.append(shape(8 * 128, 128))
        scratch = [pltpu.VMEM((8, 128), jnp.int32)]
    return pl.pallas_call(
        functools.partial(lap_kernel, lap, columns, nx_total),
        in_specs=in_specs,
        out_specs=[VMEM] * len(out_shape),
        scratch_shapes=scratch,
        out_shape=out_shape,
        compiler_params=params(),
        cost_estimate=cost(columns, 700, 6),
        name=f"lap{lap}_{columns}",
    )(*operands)


def local_call(lap, index, links, centre, right, left, aux, columns):
    return pl.pallas_call(
        functools.partial(local_kernel, lap, columns),
        in_specs=[SMEM] + [VMEM] * 5,
        out_specs=VMEM,
        out_shape=shape(columns * TILES, 8, 128),
        compiler_params=params(),
        cost_estimate=cost(columns, 450, 3),
        name=f"local{lap}_{columns}",
    )(index, centre, right, left, links, aux)


def final_call(lap, index, links, partial, above, below, before, table, start, columns, sizes, scale):
    every, told = sizes
    last = table is not None
    buffer, density = before
    operands = [index, partial, above, below, links, density]
    in_specs = [SMEM] + [VMEM] * 5
    if last:
        operands.append(table)
        in_specs.append(VMEM)
    aliases = {}
    if buffer is not None:
        aliases = {len(operands): 0}
        operands.append(buffer)
        in_specs.append(ANY)
    return pl.pallas_call(
        functools.partial(final_kernel, lap, start, columns, last, scale),
        in_specs=in_specs,
        out_specs=[ANY, VMEM],
        scratch_shapes=[
            pltpu.VMEM((columns * TILES, 8, 128), jnp.float32),
            pltpu.VMEM((8, 128), jnp.float32),
            pltpu.SemaphoreType.DMA((columns,)),
        ],
        out_shape=[
            shape(every * TILES, 8, 128),
            shape(told, 1, 128) if last else shape(8, 128),
        ],
        input_output_aliases=aliases,
        compiler_params=params(),
        cost_estimate=cost(columns, 100, 4),
        name=f"final{start}_{columns}",
    )(*operands)


def total_call(everything, count):
    return pl.pallas_call(
        total_kernel,
        in_specs=[VMEM],
        out_specs=VMEM,
        out_shape=shape(2, 1, count),
        compiler_params=params(),
        cost_estimate=pl.CostEstimate(flops=10_000, bytes_accessed=10_000, transcendentals=0),
        name="total",
    )(everything)


def passed_along(block, axis, distance):
    devices = range(lax.axis_size(axis))
    route = [((i - distance) % len(devices), i) for i in devices]
    return lax.ppermute(block, axis, route)


def exchanged(field, pulled, low, high):
    return (
        passed_along(field, "ta", -1),
        passed_along(pulled, "ta", 1),
        passed_along(low, "xyz", -1),
        passed_along(high, "xyz", 1),
    )


def body(sink, links, section_index, momenta, source):
    every = sink.shape[0]
    size = lax.axis_size("xyz")
    nx_total = sink.shape[5] * size
    whole_field = sink.reshape(every * TILES, 8, 128)
    links = links.reshape(links.shape[0], 72, 8, 128)
    laps = 3 * STEPS

    starts = [sum(CHUNKS[:i]) for i in range(len(CHUNKS))]
    made = [
        first_messages(section_index, links, whole_field, start, columns)
        for start, columns in zip(starts, CHUNKS)
    ]
    rows = first_rows(section_index, links, [raw for raw, _ in made], CHUNKS)
    state = [
        (raw, raw, exchanged(raw, pulled, *rows[2 * chunk : 2 * chunk + 2]))
        for chunk, (raw, pulled) in enumerate(made)
    ]
    table = None
    for lap in range(laps - 1):
        for chunk, columns in enumerate(CHUNKS):
            centre, aux, arrived = state[chunk]
            with_table = lap == 2 and chunk == len(CHUNKS) - 1
            phase = (nx_total, source, momenta) if with_table else None
            made = lap_call(lap, section_index, links, centre, arrived, aux, columns, phase)
            if with_table:
                *made, table = made
            field = made[0]
            if lap % 3 == 1:
                aux = made[1]
            elif lap % 3 == 2:
                aux = field
            state[chunk] = (field, aux, exchanged(field, *made[-3:]))

    scale = 1.0 / math.sqrt(576.0 * nx_total * NY * NZ)
    lap = laps - 1
    buffer, result = None, state[0][2][2]
    for chunk, (start, columns) in enumerate(zip(starts, CHUNKS)):
        centre, aux, (above, below, right, left) = state[chunk]
        partial = local_call(lap, section_index, links, centre, right, left, aux, columns)
        last = chunk == len(CHUNKS) - 1
        buffer, result = final_call(
            lap,
            section_index,
            links,
            partial,
            above,
            below,
            (buffer, result),
            table if last else None,
            start,
            columns,
            (every, size),
            scale,
        )
    everything = lax.all_to_all(result, "xyz", split_axis=0, concat_axis=0, tiled=True)
    correlator = total_call(everything, momenta.shape[0])
    return (buffer.reshape(sink.shape), correlator.reshape(2, momenta.shape[0], 1))


def solution(mesh):
    in_specs = (
        P("cfg", None, None, None, "ta", "xyz", None),
        P("cfg", None, None, None, None, "ta", "xyz", None),
        P(),
        P(),
        P(),
    )
    out_specs = (P("cfg", None, None, None, "ta", "xyz", None), P("cfg", None, "ta"))
    return jax.shard_map(body, mesh=mesh, in_specs=in_specs, out_specs=out_specs, check_vma=False)
```

```python
import functools
import math

import jax
import jax.numpy as jnp
from jax import lax
from jax.experimental import pallas as pl
from jax.experimental.pallas import tpu as pltpu
from jax.sharding import PartitionSpec as P

STEPS = 2
NY = 16
NZ = 8
TILES = 24
CHUNKS = (6, 6)
PAD = 64
VMEM_LIMIT = 16 * 1024 * 1024


flow_step = 0.05
coef_third = 0.75 * flow_step
coef_second = 8.0 * flow_step / 9.0
coef_first = 0.25 * flow_step
coef_mixed = 2.0 * flow_step / 9.0


def link_tile(links, direction, row, column):
    ref, slot = links
    at = ((direction * 3 + row) * 3 + column) * 2
    return ref[slot, at], ref[slot, at + 1]


def forward(links, direction, vector):
    out = []
    for row in range(3):
        real = imag = None
        for column in range(3):
            wr, wi = link_tile(links, direction, row, column)
            vr, vi = vector[column]
            re = wr * vr - wi * vi
            im = wr * vi + wi * vr
            real = re if real is None else real + re
            imag = im if imag is None else imag + im
        out.append((real, imag))
    return out


def backward(links, direction, vector):
    out = []
    for row in range(3):
        real = imag = None
        for column in range(3):
            wr, wi = link_tile(links, direction, column, row)
            vr, vi = vector[column]
            re = wr * vr + wi * vi
            im = wr * vi - wi * vr
            real = re if real is None else real + re
            imag = im if imag is None else imag + im
        out.append((real, imag))
    return out


def each(function, *vectors):
    return [
        tuple(function(*(vector[colour][part] for vector in vectors)) for part in range(2))
        for colour in range(3)
    ]


def tiles_of(ref, base):
    return [(ref[base + 2 * colour], ref[base + 2 * colour + 1]) for colour in range(3)]


def rows_of(ref, base):
    return [
        tuple(
            jnp.broadcast_to(ref[pl.ds(base + 2 * colour + part, 1), :], (8, 128))
            for part in range(2)
        )
        for colour in range(3)
    ]


def put_tiles(ref, base, vector):
    for colour in range(3):
        for part in range(2):
            ref[base + 2 * colour + part] = vector[colour][part]


def put_rows(ref, base, vector, row):
    for colour in range(3):
        for part in range(2):
            ref[pl.ds(base + 2 * colour + part, 1), :] = vector[colour][part][row : row + 1, :]


def roll(value, shift, axis):
    return pltpu.roll(value, shift % value.shape[axis], axis)


def messages(links, base, field, pulled_ref, low_ref, high_ref):
    put_tiles(pulled_ref, base, backward(links, 0, field))
    put_rows(low_ref, base, field, 0)
    put_rows(high_ref, base, backward(links, 1, field), 7)


def each_vector(columns):
    def loop(work):
        @pl.loop(0, columns)
        def _(column):
            for spin in range(4):
                work(spin, pl.multiple_of(column * TILES, TILES) + 6 * spin)

    return loop


def first_kernel(
    start, columns, index_ref, field_ref, links_ref, raw_ref, pulled_ref, slots_ref, next_ref, sems
):
    def copy_in(column):
        return pltpu.make_async_copy(
            field_ref.at[pl.ds((start + column) * TILES, TILES)],
            raw_ref.at[pl.ds(column * TILES, TILES)],
            sems.at[column],
        )

    index_copy = pltpu.make_async_copy(index_ref, slots_ref, sems.at[columns])
    link_copy = pltpu.make_async_copy(
        links_ref.at[:, pl.ds(0, 18)], next_ref, sems.at[columns + 1]
    )
    index_copy.start()
    link_copy.start()
    for column in range(columns):
        copy_in(column).start()
    index_copy.wait()
    link_copy.wait()
    links = (next_ref, slot_of(slots_ref, 0))

    @pl.loop(0, columns)
    def _(column):
        copy_in(column).wait()
        for spin in range(4):
            base = pl.multiple_of(column * TILES, TILES) + 6 * spin
            put_tiles(pulled_ref, base, backward(links, 0, tiles_of(raw_ref, base)))


def first_rows_kernel(sizes, index_ref, links_ref, *refs):
    links = (links_ref, slot_of(index_ref, 0))
    for chunk, columns in enumerate(sizes):
        raw_ref = refs[chunk]
        low_ref, high_ref = refs[len(sizes) + 2 * chunk : len(sizes) + 2 * chunk + 2]

        @each_vector(columns)
        def _(spin, base):
            field = tiles_of(raw_ref, base)
            put_rows(low_ref, base, field, 0)
            put_rows(high_ref, base, backward(links, 1, field), 7)


def local_terms(base, centre, right_ref, left_ref, links, masks, total):
    is_top, is_bottom, is_far, is_near = masks
    add = functools.partial(each, lambda a, b: a + b)
    above_x = each(
        lambda v, h: jnp.where(is_top, h, roll(v, -1, 0)), centre, rows_of(right_ref, base)
    )
    total = add(total, forward(links, 1, above_x))
    below_x = each(
        lambda v, h: jnp.where(is_bottom, h, roll(v, 1, 0)),
        backward(links, 1, centre),
        rows_of(left_ref, base),
    )
    total = add(total, below_x)
    total = add(total, forward(links, 2, each(lambda v: roll(v, -NZ, 1), centre)))
    total = add(total, each(lambda v: roll(v, NZ, 1), backward(links, 2, centre)))
    above_z = each(lambda v: jnp.where(is_far, roll(v, NZ - 1, 1), roll(v, -1, 1)), centre)
    total = add(total, forward(links, 3, above_z))
    below_z = each(
        lambda v: jnp.where(is_near, roll(v, 1 - NZ, 1), roll(v, 1, 1)),
        backward(links, 3, centre),
    )
    return add(total, below_z)


def edge_masks():
    sub = lax.broadcasted_iota(jnp.int32, (8, 128), 0)
    zcoord = lax.broadcasted_iota(jnp.int32, (8, 128), 1) % NZ
    return sub == 7, sub == 0, zcoord == NZ - 1, zcoord == 0


def lap_kernel(lap, columns, nx_total, index_ref, *refs):
    kind = lap % 3
    refs = list(refs)
    centre_ref, above_ref, below_ref, right_ref, left_ref, links_ref = refs[:6]
    refs = refs[6:]
    aux_ref = refs.pop(0) if kind > 0 else None
    if nx_total:
        source_ref, momenta_ref = refs[:2]
        refs = refs[2:]
        both_ref = refs.pop()
        phases(nx_total, source_ref, momenta_ref, refs.pop(), both_ref)
    out_ref = refs.pop(0)
    sum_ref = refs.pop(0) if kind == 1 else None
    pulled_ref, low_ref, high_ref = refs

    links = (links_ref, slot_of(index_ref, lap))
    links_next = (links_ref, slot_of(index_ref, lap + 1))
    masks = edge_masks()
    add = functools.partial(each, lambda a, b: a + b)

    @each_vector(columns)
    def _(spin, base):
        centre = tiles_of(centre_ref, base)
        total = each(lambda v, p: p - 8.0 * v, centre, tiles_of(below_ref, base))
        total = add(total, forward(links, 0, tiles_of(above_ref, base)))
        total = local_terms(base, centre, right_ref, left_ref, links, masks, total)
        if kind == 0:
            field = each(lambda t: coef_third * t, total)
        elif kind == 1:
            middle = each(lambda a, t: a + coef_second * t, tiles_of(aux_ref, base), total)
            field = each(lambda m, v: coef_first * m - coef_mixed * v, middle, centre)
            put_tiles(sum_ref, base, add(middle, centre))
        else:
            field = add(tiles_of(aux_ref, base), total)
        put_tiles(out_ref, base, field)
        messages(links_next, base, field, pulled_ref, low_ref, high_ref)


def local_kernel(
    lap, columns, index_ref, centre_ref, right_ref, left_ref, links_ref, aux_ref, out_ref
):
    links = (links_ref, slot_of(index_ref, lap))
    masks = edge_masks()

    @each_vector(columns)
    def _(spin, base):
        centre = tiles_of(centre_ref, base)
        total = each(lambda v, a: a - 8.0 * v, centre, tiles_of(aux_ref, base))
        total = local_terms(base, centre, right_ref, left_ref, links, masks, total)
        put_tiles(out_ref, base, total)


def final_kernel(lap, start, columns, last, scale, index_ref, *refs):
    refs = list(refs)
    partial_ref, above_ref, below_ref, links_ref, before_ref = refs[:5]
    table_ref = refs[5] if last else None
    out_ref, result_ref, held_ref, total_ref, sems = refs[-5:]
    links = (links_ref, slot_of(index_ref, lap))
    total_ref[...] = before_ref[...] if start else jnp.zeros((8, 128), jnp.float32)

    def copy_out(column):
        return pltpu.make_async_copy(
            held_ref.at[pl.ds(column * TILES, TILES)],
            out_ref.at[pl.ds((start + column) * TILES, TILES)],
            sems.at[column],
        )

    @pl.loop(0, columns)
    def _(column):
        density = total_ref[...]
        for spin in range(4):
            base = pl.multiple_of(column * TILES, TILES) + 6 * spin
            total = each(lambda a, b: a + b, tiles_of(partial_ref, base), tiles_of(below_ref, base))
            field = each(
                lambda a, b: a + b, total, forward(links, 0, tiles_of(above_ref, base))
            )
            put_tiles(held_ref, base, field)
            part = None
            for colour in range(3):
                for value in field[colour]:
                    part = value * value if part is None else part + value * value
            density = density + part if spin < 2 else density - part
        total_ref[...] = density
        copy_out(column).start()

    if last:
        sums = None
        for row in range(8):
            phase = table_ref[pl.ds(row * 128, 128), :]
            term = lax.dot_general(
                jnp.broadcast_to(total_ref[row : row + 1, :] * scale, (8, 128)),
                phase,
                (((1,), (0,)), ((), ())),
                precision=lax.Precision.HIGHEST,
                preferred_element_type=jnp.float32,
            )
            sums = term if sums is None else sums + term
        for row in range(result_ref.shape[0]):
            result_ref[row] = sums[0:1, :]
    else:
        result_ref[...] = total_ref[...]

    @pl.loop(0, columns)
    def _(column):
        copy_out(column).wait()


def phases(nx_total, source_ref, momenta_ref, table_ref, both_ref):
    count = momenta_ref.shape[1]
    both_ref[...] = jnp.zeros(both_ref.shape, jnp.int32)
    both_ref[0:3, 0:count] = momenta_ref[...]
    both = both_ref[...]
    both_ref[...] = both + roll(both, PAD, 1)
    sites = lax.broadcasted_iota(jnp.int32, (128, 128), 0)
    quarter = jnp.where(lax.broadcasted_iota(jnp.int32, (128, 128), 1) >= PAD, 0.25, 0.0)

    def within(value, size):
        return jnp.bitwise_and(value, size - 1)

    def fraction(axis, distance, size):
        momentum = jnp.broadcast_to(both_ref[axis : axis + 1, :], (128, 128))
        return within(momentum * within(distance, size), size).astype(jnp.float32) * (1.0 / size)

    plane = fraction(1, sites // NZ - source_ref[1], NY) + quarter
    plane = plane + fraction(2, within(sites, NZ) - source_ref[2], NZ)
    first = lax.axis_index("xyz") * 8

    @pl.loop(0, 8)
    def _(row):
        xcoord = jnp.full((128, 128), first + row - source_ref[0], jnp.int32)
        turns = plane + fraction(0, xcoord, nx_total)
        turns = turns - jnp.floor(turns)
        table_ref[pl.ds(pl.multiple_of(row * 128, 128), 128), :] = jnp.cos(2.0 * math.pi * turns)


def total_kernel(all_ref, out_ref):
    count = out_ref.shape[2]
    total = jnp.sum(all_ref[...], axis=0)
    out_ref[0] = total[:, 0:count]
    out_ref[1] = total[:, PAD : PAD + count]


def slot_of(index, lap):
    return index[STEPS - 1 - lap // 3, 2 - lap % 3]


def shape(*dims):
    return jax.ShapeDtypeStruct(dims, jnp.float32)


def cost(columns, per_spin, arrays):
    return pl.CostEstimate(
        flops=columns * 4 * per_spin * 1024,
        bytes_accessed=columns * TILES * 4096 * arrays,
        transcendentals=0,
    )


def params():
    return pltpu.CompilerParams(vmem_limit_bytes=VMEM_LIMIT)


SMEM = pl.BlockSpec(memory_space=pltpu.SMEM)
VMEM = pl.BlockSpec(memory_space=pltpu.VMEM)
ANY = pl.BlockSpec(memory_space=pl.ANY)


def first_messages(index, links, field, start, columns):
    return pl.pallas_call(
        functools.partial(first_kernel, start, columns),
        in_specs=[ANY] * 3,
        out_specs=[VMEM] * 2,
        scratch_shapes=[
            pltpu.SMEM(index.shape, jnp.int32),
            pltpu.VMEM((links.shape[0], 18, 8, 128), jnp.float32),
            pltpu.SemaphoreType.DMA((columns + 2,)),
        ],
        out_shape=[shape(columns * TILES, 8, 128)] * 2,
        compiler_params=params(),
        cost_estimate=cost(columns, 70, 2),
        name="first_messages",
    )(*(pltpu.with_memory_space_constraint(a, pltpu.HBM) for a in (index, field, links)))


def first_rows(index, links, fields, sizes):
    shapes = [shape(columns * TILES, 128) for columns in sizes for _ in range(2)]
    return pl.pallas_call(
        functools.partial(first_rows_kernel, sizes),
        in_specs=[SMEM] + [VMEM] * (1 + len(fields)),
        out_specs=[VMEM] * len(shapes),
        out_shape=shapes,
        compiler_params=params(),
        cost_estimate=cost(sum(sizes), 70, 1),
        name="first_rows",
    )(index, links, *fields)


def lap_call(lap, index, links, centre, arrived, aux, columns, phase=None):
    kind = lap % 3
    operands = [index, centre, *arrived, links]
    if kind > 0:
        operands.append(aux)
    in_specs = [SMEM] + [VMEM] * (len(operands) - 1)
    fields = 3 if kind == 1 else 2
    out_shape = [shape(columns * TILES, 8, 128)] * fields + [shape(columns * TILES, 128)] * 2
    scratch, nx_total = [], 0
    if phase is not None:
        nx_total, source, momenta = phase
        operands += [source, momenta.T]
        in_specs += [SMEM, VMEM]
        out_shape.append(shape(8 * 128, 128))
        scratch = [pltpu.VMEM((8, 128), jnp.int32)]
    return pl.pallas_call(
        functools.partial(lap_kernel, lap, columns, nx_total),
        in_specs=in_specs,
        out_specs=[VMEM] * len(out_shape),
        scratch_shapes=scratch,
        out_shape=out_shape,
        compiler_params=params(),
        cost_estimate=cost(columns, 700, 6),
    )(*operands)


def local_call(lap, index, links, centre, right, left, aux, columns):
    return pl.pallas_call(
        functools.partial(local_kernel, lap, columns),
        in_specs=[SMEM] + [VMEM] * 5,
        out_specs=VMEM,
        out_shape=shape(columns * TILES, 8, 128),
        compiler_params=params(),
        cost_estimate=cost(columns, 450, 3),
    )(index, centre, right, left, links, aux)


def final_call(lap, index, links, partial, above, below, before, table, start, columns, sizes, scale):
    every, told = sizes
    last = table is not None
    buffer, density = before
    operands = [index, partial, above, below, links, density]
    in_specs = [SMEM] + [VMEM] * 5
    if last:
        operands.append(table)
        in_specs.append(VMEM)
    aliases = {}
    if buffer is not None:
        aliases = {len(operands): 0}
        operands.append(buffer)
        in_specs.append(ANY)
    return pl.pallas_call(
        functools.partial(final_kernel, lap, start, columns, last, scale),
        in_specs=in_specs,
        out_specs=[ANY, VMEM],
        scratch_shapes=[
            pltpu.VMEM((columns * TILES, 8, 128), jnp.float32),
            pltpu.VMEM((8, 128), jnp.float32),
            pltpu.SemaphoreType.DMA((columns,)),
        ],
        out_shape=[
            shape(every * TILES, 8, 128),
            shape(told, 1, 128) if last else shape(8, 128),
        ],
        input_output_aliases=aliases,
        compiler_params=params(),
        cost_estimate=cost(columns, 100, 4),
    )(*operands)


def total_call(everything, count):
    return pl.pallas_call(
        total_kernel,
        in_specs=[VMEM],
        out_specs=VMEM,
        out_shape=shape(2, 1, count),
        compiler_params=params(),
        cost_estimate=pl.CostEstimate(flops=10_000, bytes_accessed=10_000, transcendentals=0),
        name="total",
    )(everything)


def passed_along(block, axis, distance):
    devices = range(lax.axis_size(axis))
    route = [((i - distance) % len(devices), i) for i in devices]
    return lax.ppermute(block, axis, route)


def exchanged(field, pulled, low, high):
    above = passed_along(field, "ta", -1)
    below = passed_along(pulled, "ta", 1)
    right = passed_along(low, "xyz", -1)
    left = passed_along(high, "xyz", 1)
    return above, below, right, left


def body(sink, links, section_index, momenta, source):
    every = sink.shape[0]
    size = lax.axis_size("xyz")
    nx_total = sink.shape[5] * size
    whole_field = sink.reshape(every * TILES, 8, 128)
    links = links.reshape(links.shape[0], 72, 8, 128)
    laps = 3 * STEPS

    starts = [sum(CHUNKS[:i]) for i in range(len(CHUNKS))]
    made = [
        first_messages(section_index, links, whole_field, start, columns)
        for start, columns in zip(starts, CHUNKS)
    ]
    rows = first_rows(section_index, links, [raw for raw, _ in made], CHUNKS)
    state = [
        (raw, raw, exchanged(raw, pulled, *rows[2 * chunk : 2 * chunk + 2]))
        for chunk, (raw, pulled) in enumerate(made)
    ]
    table = None
    for lap in range(laps - 1):
        for chunk, columns in enumerate(CHUNKS):
            centre, aux, arrived = state[chunk]
            with_table = lap == 2 and chunk == len(CHUNKS) - 1
            phase = (nx_total, source, momenta) if with_table else None
            made = lap_call(lap, section_index, links, centre, arrived, aux, columns, phase)
            if with_table:
                *made, table = made
            field = made[0]
            if lap % 3 == 1:
                aux = made[1]
            elif lap % 3 == 2:
                aux = field
            state[chunk] = (field, aux, exchanged(field, *made[-3:]))

    scale = 1.0 / math.sqrt(576.0 * nx_total * NY * NZ)
    lap = laps - 1
    buffer, result = None, state[0][2][2]
    for chunk, (start, columns) in enumerate(zip(starts, CHUNKS)):
        centre, aux, (above, below, right, left) = state[chunk]
        partial = local_call(lap, section_index, links, centre, right, left, aux, columns)
        last = chunk == len(CHUNKS) - 1
        buffer, result = final_call(
            lap,
            section_index,
            links,
            partial,
            above,
            below,
            (buffer, result),
            table if last else None,
            start,
            columns,
            (every, size),
            scale,
        )
    everything = lax.all_to_all(result, "xyz", split_axis=0, concat_axis=0, tiled=True)
    correlator = total_call(everything, momenta.shape[0])
    return (buffer.reshape(sink.shape), correlator.reshape(2, momenta.shape[0], 1))


def solution(mesh):
    in_specs = (
        P("cfg", None, None, None, "ta", "xyz", None),
        P("cfg", None, None, None, None, "ta", "xyz", None),
        P(),
        P(),
        P(),
    )
    out_specs = (P("cfg", None, None, None, "ta", "xyz", None), P("cfg", None, "ta"))
    return jax.shard_map(body, mesh=mesh, in_specs=in_specs, out_specs=out_specs, check_vma=False)
```

```python
import functools
import math

import jax
import jax.numpy as jnp
from jax import lax
from jax.experimental import pallas as pl
from jax.experimental.pallas import tpu as pltpu
from jax.sharding import PartitionSpec as P

STEPS = 2
NY = 16
NZ = 8
TILES = 24
CHUNKS = (6, 6)
PAD = 64
VMEM_LIMIT = 16 * 1024 * 1024


flow_step = 0.05
coef_third = 0.75 * flow_step
coef_second = 8.0 * flow_step / 9.0
coef_first = 0.25 * flow_step
coef_mixed = 2.0 * flow_step / 9.0


def link_tile(links, direction, row, column):
    ref, slot = links
    at = ((direction * 3 + row) * 3 + column) * 2
    return ref[slot, at], ref[slot, at + 1]


def forward(links, direction, vector):
    out = []
    for row in range(3):
        real = imag = None
        for column in range(3):
            wr, wi = link_tile(links, direction, row, column)
            vr, vi = vector[column]
            re = wr * vr - wi * vi
            im = wr * vi + wi * vr
            real = re if real is None else real + re
            imag = im if imag is None else imag + im
        out.append((real, imag))
    return out


def backward(links, direction, vector):
    out = []
    for row in range(3):
        real = imag = None
        for column in range(3):
            wr, wi = link_tile(links, direction, column, row)
            vr, vi = vector[column]
            re = wr * vr + wi * vi
            im = wr * vi - wi * vr
            real = re if real is None else real + re
            imag = im if imag is None else imag + im
        out.append((real, imag))
    return out


def each(function, *vectors):
    return [
        tuple(function(*(vector[colour][part] for vector in vectors)) for part in range(2))
        for colour in range(3)
    ]


def tiles_of(ref, base):
    return [(ref[base + 2 * colour], ref[base + 2 * colour + 1]) for colour in range(3)]


def rows_of(ref, base):
    return [
        tuple(
            jnp.broadcast_to(ref[pl.ds(base + 2 * colour + part, 1), :], (8, 128))
            for part in range(2)
        )
        for colour in range(3)
    ]


def put_tiles(ref, base, vector):
    for colour in range(3):
        for part in range(2):
            ref[base + 2 * colour + part] = vector[colour][part]


def put_rows(ref, base, vector, row):
    for colour in range(3):
        for part in range(2):
            ref[pl.ds(base + 2 * colour + part, 1), :] = vector[colour][part][row : row + 1, :]


def roll(value, shift, axis):
    return pltpu.roll(value, shift % value.shape[axis], axis)


def messages(links, base, field, pulled_ref, low_ref, high_ref):
    put_tiles(pulled_ref, base, backward(links, 0, field))
    put_rows(low_ref, base, field, 0)
    put_rows(high_ref, base, backward(links, 1, field), 7)


def each_vector(columns):
    def loop(work):
        @pl.loop(0, columns)
        def _(column):
            for spin in range(4):
                work(spin, pl.multiple_of(column * TILES, TILES) + 6 * spin)

    return loop


def first_kernel(
    start, columns, index_ref, field_ref, links_ref, raw_ref, pulled_ref, slots_ref, next_ref, sems
):
    def copy_in(column):
        return pltpu.make_async_copy(
            field_ref.at[pl.ds((start + column) * TILES, TILES)],
            raw_ref.at[pl.ds(column * TILES, TILES)],
            sems.at[column],
        )

    index_copy = pltpu.make_async_copy(index_ref, slots_ref, sems.at[columns])
    link_copy = pltpu.make_async_copy(
        links_ref.at[:, pl.ds(0, 18)], next_ref, sems.at[columns + 1]
    )
    index_copy.start()
    link_copy.start()
    for column in range(columns):
        copy_in(column).start()
    index_copy.wait()
    link_copy.wait()
    links = (next_ref, slot_of(slots_ref, 0))

    @pl.loop(0, columns)
    def _(column):
        copy_in(column).wait()
        for spin in range(4):
            base = pl.multiple_of(column * TILES, TILES) + 6 * spin
            put_tiles(pulled_ref, base, backward(links, 0, tiles_of(raw_ref, base)))


def first_rows_kernel(sizes, index_ref, links_ref, *refs):
    links = (links_ref, slot_of(index_ref, 0))
    for chunk, columns in enumerate(sizes):
        raw_ref = refs[chunk]
        low_ref, high_ref = refs[len(sizes) + 2 * chunk : len(sizes) + 2 * chunk + 2]

        @each_vector(columns)
        def _(spin, base):
            field = tiles_of(raw_ref, base)
            put_rows(low_ref, base, field, 0)
            put_rows(high_ref, base, backward(links, 1, field), 7)


def local_terms(base, centre, right_ref, left_ref, links, masks, total):
    is_top, is_bottom, is_far, is_near = masks
    add = functools.partial(each, lambda a, b: a + b)
    above_x = each(
        lambda v, h: jnp.where(is_top, h, roll(v, -1, 0)), centre, rows_of(right_ref, base)
    )
    total = add(total, forward(links, 1, above_x))
    below_x = each(
        lambda v, h: jnp.where(is_bottom, h, roll(v, 1, 0)),
        backward(links, 1, centre),
        rows_of(left_ref, base),
    )
    total = add(total, below_x)
    total = add(total, forward(links, 2, each(lambda v: roll(v, -NZ, 1), centre)))
    total = add(total, each(lambda v: roll(v, NZ, 1), backward(links, 2, centre)))
    above_z = each(lambda v: jnp.where(is_far, roll(v, NZ - 1, 1), roll(v, -1, 1)), centre)
    total = add(total, forward(links, 3, above_z))
    below_z = each(
        lambda v: jnp.where(is_near, roll(v, 1 - NZ, 1), roll(v, 1, 1)),
        backward(links, 3, centre),
    )
    return add(total, below_z)


def edge_masks():
    sub = lax.broadcasted_iota(jnp.int32, (8, 128), 0)
    zcoord = lax.broadcasted_iota(jnp.int32, (8, 128), 1) % NZ
    return sub == 7, sub == 0, zcoord == NZ - 1, zcoord == 0


def lap_kernel(lap, columns, nx_total, index_ref, *refs):
    kind = lap % 3
    refs = list(refs)
    centre_ref, above_ref, below_ref, right_ref, left_ref, links_ref = refs[:6]
    refs = refs[6:]
    aux_ref = refs.pop(0) if kind > 0 else None
    if nx_total:
        source_ref, momenta_ref = refs[:2]
        refs = refs[2:]
        both_ref = refs.pop()
        phases(nx_total, source_ref, momenta_ref, refs.pop(), both_ref)
    out_ref = refs.pop(0)
    sum_ref = refs.pop(0) if kind == 1 else None
    pulled_ref, low_ref, high_ref = refs

    links = (links_ref, slot_of(index_ref, lap))
    links_next = (links_ref, slot_of(index_ref, lap + 1))
    masks = edge_masks()
    add = functools.partial(each, lambda a, b: a + b)

    @each_vector(columns)
    def _(spin, base):
        centre = tiles_of(centre_ref, base)
        total = each(lambda v, p: p - 8.0 * v, centre, tiles_of(below_ref, base))
        total = add(total, forward(links, 0, tiles_of(above_ref, base)))
        total = local_terms(base, centre, right_ref, left_ref, links, masks, total)
        if kind == 0:
            field = each(lambda t: coef_third * t, total)
        elif kind == 1:
            middle = each(lambda a, t: a + coef_second * t, tiles_of(aux_ref, base), total)
            field = each(lambda m, v: coef_first * m - coef_mixed * v, middle, centre)
            put_tiles(sum_ref, base, add(middle, centre))
        else:
            field = add(tiles_of(aux_ref, base), total)
        put_tiles(out_ref, base, field)
        messages(links_next, base, field, pulled_ref, low_ref, high_ref)


def local_kernel(
    lap, columns, index_ref, centre_ref, right_ref, left_ref, links_ref, aux_ref, out_ref
):
    links = (links_ref, slot_of(index_ref, lap))
    masks = edge_masks()

    @each_vector(columns)
    def _(spin, base):
        centre = tiles_of(centre_ref, base)
        total = each(lambda v, a: a - 8.0 * v, centre, tiles_of(aux_ref, base))
        total = local_terms(base, centre, right_ref, left_ref, links, masks, total)
        put_tiles(out_ref, base, total)


def final_kernel(lap, start, columns, last, scale, index_ref, *refs):
    refs = list(refs)
    partial_ref, above_ref, below_ref, links_ref, before_ref = refs[:5]
    table_ref = refs[5] if last else None
    out_ref, result_ref, held_ref, total_ref, sems = refs[-5:]
    held_ref = out_ref if last else held_ref
    links = (links_ref, slot_of(index_ref, lap))
    total_ref[...] = before_ref[...] if start else jnp.zeros((8, 128), jnp.float32)

    def copy_out(column):
        return pltpu.make_async_copy(
            held_ref.at[pl.ds(column * TILES, TILES)],
            out_ref.at[pl.ds((start + column) * TILES, TILES)],
            sems.at[column],
        )

    @pl.loop(0, columns)
    def _(column):
        density = total_ref[...]
        for spin in range(4):
            base = pl.multiple_of(column * TILES, TILES) + 6 * spin
            total = each(lambda a, b: a + b, tiles_of(partial_ref, base), tiles_of(below_ref, base))
            field = each(
                lambda a, b: a + b, total, forward(links, 0, tiles_of(above_ref, base))
            )
            put_tiles(held_ref, base, field)
            part = None
            for colour in range(3):
                for value in field[colour]:
                    part = value * value if part is None else part + value * value
            density = density + part if spin < 2 else density - part
        total_ref[...] = density
        if not last:
            copy_out(column).start()

    if last:
        sums = None
        for row in range(8):
            phase = table_ref[pl.ds(row * 128, 128), :]
            term = lax.dot_general(
                jnp.broadcast_to(total_ref[row : row + 1, :] * scale, (8, 128)),
                phase,
                (((1,), (0,)), ((), ())),
                precision=lax.Precision.HIGHEST,
                preferred_element_type=jnp.float32,
            )
            sums = term if sums is None else sums + term
        for row in range(result_ref.shape[0]):
            result_ref[row] = sums[0:1, :]
    else:
        result_ref[...] = total_ref[...]

        @pl.loop(0, columns)
        def _(column):
            copy_out(column).wait()


def phases(nx_total, source_ref, momenta_ref, table_ref, both_ref):
    count = momenta_ref.shape[1]
    both_ref[...] = jnp.zeros(both_ref.shape, jnp.int32)
    both_ref[0:3, 0:count] = momenta_ref[...]
    both = both_ref[...]
    both_ref[...] = both + roll(both, PAD, 1)
    sites = lax.broadcasted_iota(jnp.int32, (128, 128), 0)
    quarter = jnp.where(lax.broadcasted_iota(jnp.int32, (128, 128), 1) >= PAD, 0.25, 0.0)

    def within(value, size):
        return jnp.bitwise_and(value, size - 1)

    def fraction(axis, distance, size):
        momentum = jnp.broadcast_to(both_ref[axis : axis + 1, :], (128, 128))
        return within(momentum * within(distance, size), size).astype(jnp.float32) * (1.0 / size)

    plane = fraction(1, sites // NZ - source_ref[1], NY) + quarter
    plane = plane + fraction(2, within(sites, NZ) - source_ref[2], NZ)
    first = lax.axis_index("xyz") * 8

    @pl.loop(0, 8)
    def _(row):
        xcoord = jnp.full((128, 128), first + row - source_ref[0], jnp.int32)
        turns = plane + fraction(0, xcoord, nx_total)
        turns = turns - jnp.floor(turns)
        table_ref[pl.ds(pl.multiple_of(row * 128, 128), 128), :] = jnp.cos(2.0 * math.pi * turns)


def total_kernel(start, columns, all_ref, held_ref, buffer_ref, field_ref, out_ref, sem):
    copy = pltpu.make_async_copy(
        held_ref, field_ref.at[pl.ds(start * TILES, columns * TILES)], sem.at[0]
    )
    copy.start()
    count = out_ref.shape[2]
    total = jnp.sum(all_ref[...], axis=0)
    out_ref[0] = total[:, 0:count]
    out_ref[1] = total[:, PAD : PAD + count]
    copy.wait()


def slot_of(index, lap):
    return index[STEPS - 1 - lap // 3, 2 - lap % 3]


def shape(*dims):
    return jax.ShapeDtypeStruct(dims, jnp.float32)


def cost(columns, per_spin, arrays):
    return pl.CostEstimate(
        flops=columns * 4 * per_spin * 1024,
        bytes_accessed=columns * TILES * 4096 * arrays,
        transcendentals=0,
    )


def params():
    return pltpu.CompilerParams(vmem_limit_bytes=VMEM_LIMIT)


def whole_spec():
    return pl.BlockSpec(memory_space=pltpu.VMEM)


SMEM = pl.BlockSpec(memory_space=pltpu.SMEM)
VMEM = pl.BlockSpec(memory_space=pltpu.VMEM)
ANY = pl.BlockSpec(memory_space=pl.ANY)


def first_messages(index, links, field, start, columns):
    return pl.pallas_call(
        functools.partial(first_kernel, start, columns),
        in_specs=[ANY] * 3,
        out_specs=[VMEM] * 2,
        scratch_shapes=[
            pltpu.SMEM(index.shape, jnp.int32),
            pltpu.VMEM((links.shape[0], 18, 8, 128), jnp.float32),
            pltpu.SemaphoreType.DMA((columns + 2,)),
        ],
        out_shape=[shape(columns * TILES, 8, 128)] * 2,
        compiler_params=params(),
        cost_estimate=cost(columns, 70, 2),
        name="first_messages",
    )(*(pltpu.with_memory_space_constraint(a, pltpu.HBM) for a in (index, field, links)))


def first_rows(index, links, fields, sizes):
    shapes = [shape(columns * TILES, 128) for columns in sizes for _ in range(2)]
    return pl.pallas_call(
        functools.partial(first_rows_kernel, sizes),
        in_specs=[SMEM] + [VMEM] * (1 + len(fields)),
        out_specs=[VMEM] * len(shapes),
        out_shape=shapes,
        compiler_params=params(),
        cost_estimate=cost(sum(sizes), 70, 1),
        name="first_rows",
    )(index, links, *fields)


def lap_call(lap, index, links, centre, arrived, aux, columns, phase=None):
    kind = lap % 3
    operands = [index, centre, *arrived, links]
    if kind > 0:
        operands.append(aux)
    in_specs = [SMEM] + [VMEM] * (len(operands) - 1)
    fields = 3 if kind == 1 else 2
    out_shape = [shape(columns * TILES, 8, 128)] * fields + [shape(columns * TILES, 128)] * 2
    scratch, nx_total = [], 0
    if phase is not None:
        nx_total, source, momenta = phase
        operands += [source, momenta.T]
        in_specs += [SMEM, VMEM]
        out_shape.append(shape(8 * 128, 128))
        scratch = [pltpu.VMEM((8, 128), jnp.int32)]
    return pl.pallas_call(
        functools.partial(lap_kernel, lap, columns, nx_total),
        in_specs=in_specs,
        out_specs=[VMEM] * len(out_shape),
        scratch_shapes=scratch,
        out_shape=out_shape,
        compiler_params=params(),
        cost_estimate=cost(columns, 700, 6),
        name=f"lap{lap}_{columns}",
    )(*operands)


def local_call(lap, index, links, centre, right, left, aux, columns):
    return pl.pallas_call(
        functools.partial(local_kernel, lap, columns),
        in_specs=[SMEM] + [VMEM] * 5,
        out_specs=VMEM,
        out_shape=shape(columns * TILES, 8, 128),
        compiler_params=params(),
        cost_estimate=cost(columns, 450, 3),
        name=f"local{lap}_{columns}",
    )(index, centre, right, left, links, aux)


def final_call(lap, index, links, partial, above, below, before, table, start, columns, sizes, scale):
    every, told = sizes
    last = table is not None
    buffer, density = before
    held = 1 if last else columns * TILES
    operands = [index, partial, above, below, links, density]
    in_specs = [SMEM] + [VMEM] * 5
    if last:
        operands.append(table)
        in_specs.append(VMEM)
    aliases = {}
    if buffer is not None and not last:
        aliases = {len(operands): 0}
        operands.append(buffer)
        in_specs.append(ANY)
    return pl.pallas_call(
        functools.partial(final_kernel, lap, start, columns, last, scale),
        in_specs=in_specs,
        out_specs=[VMEM if last else ANY, VMEM],
        scratch_shapes=[
            pltpu.VMEM((held, 8, 128), jnp.float32),
            pltpu.VMEM((8, 128), jnp.float32),
            pltpu.SemaphoreType.DMA((columns,)),
        ],
        out_shape=[
            shape((columns if last else every) * TILES, 8, 128),
            shape(told, 1, 128) if last else shape(8, 128),
        ],
        input_output_aliases=aliases,
        compiler_params=params(),
        cost_estimate=cost(columns, 100, 4),
        name=f"final{start}_{columns}",
    )(*operands)


def total_call(everything, held, buffer, start, columns, count):
    return pl.pallas_call(
        functools.partial(total_kernel, start, columns),
        in_specs=[VMEM, VMEM, ANY],
        out_specs=[ANY, VMEM],
        out_shape=[jax.ShapeDtypeStruct(buffer.shape, buffer.dtype), shape(2, 1, count)],
        scratch_shapes=[pltpu.SemaphoreType.DMA((1,))],
        input_output_aliases={2: 0},
        compiler_params=params(),
        cost_estimate=pl.CostEstimate(flops=10_000, bytes_accessed=10_000, transcendentals=0),
        name="total",
    )(everything, held, buffer)


def passed_along(block, axis, distance):
    devices = range(lax.axis_size(axis))
    route = [((i - distance) % len(devices), i) for i in devices]
    return lax.ppermute(block, axis, route)


def exchanged(field, pulled, low, high):
    return (
        passed_along(field, "ta", -1),
        passed_along(pulled, "ta", 1),
        passed_along(low, "xyz", -1),
        passed_along(high, "xyz", 1),
    )


def body(sink, links, section_index, momenta, source):
    every = sink.shape[0]
    size = lax.axis_size("xyz")
    nx_total = sink.shape[5] * size
    whole_field = sink.reshape(every * TILES, 8, 128)
    links = links.reshape(links.shape[0], 72, 8, 128)
    laps = 3 * STEPS

    starts = [sum(CHUNKS[:i]) for i in range(len(CHUNKS))]
    made = [
        first_messages(section_index, links, whole_field, start, columns)
        for start, columns in zip(starts, CHUNKS)
    ]
    rows = first_rows(section_index, links, [raw for raw, _ in made], CHUNKS)
    state = [
        (raw, raw, exchanged(raw, pulled, *rows[2 * chunk : 2 * chunk + 2]))
        for chunk, (raw, pulled) in enumerate(made)
    ]
    table = None
    for lap in range(laps - 1):
        for chunk, columns in enumerate(CHUNKS):
            centre, aux, arrived = state[chunk]
            with_table = lap == 2 and chunk == len(CHUNKS) - 1
            phase = (nx_total, source, momenta) if with_table else None
            made = lap_call(lap, section_index, links, centre, arrived, aux, columns, phase)
            if with_table:
                *made, table = made
            field = made[0]
            if lap % 3 == 1:
                aux = made[1]
            elif lap % 3 == 2:
                aux = field
            state[chunk] = (field, aux, exchanged(field, *made[-3:]))

    scale = 1.0 / math.sqrt(576.0 * nx_total * NY * NZ)
    lap = laps - 1
    buffer, result = None, state[0][2][2]
    for chunk, (start, columns) in enumerate(zip(starts, CHUNKS)):
        centre, aux, (above, below, right, left) = state[chunk]
        partial = local_call(lap, section_index, links, centre, right, left, aux, columns)
        last = chunk == len(CHUNKS) - 1
        made, result = final_call(
            lap,
            section_index,
            links,
            partial,
            above,
            below,
            (buffer, result),
            table if last else None,
            start,
            columns,
            (every, size),
            scale,
        )
        if not last:
            buffer = made
    everything = lax.all_to_all(result, "xyz", split_axis=0, concat_axis=0, tiled=True)
    buffer, correlator = total_call(everything, made, buffer, start, columns, momenta.shape[0])
    return (buffer.reshape(sink.shape), correlator.reshape(2, momenta.shape[0], 1))


def solution(mesh):
    in_specs = (
        P("cfg", None, None, None, "ta", "xyz", None),
        P("cfg", None, None, None, None, "ta", "xyz", None),
        P(),
        P(),
        P(),
    )
    out_specs = (P("cfg", None, None, None, "ta", "xyz", None), P("cfg", None, "ta"))
    return jax.shard_map(body, mesh=mesh, in_specs=in_specs, out_specs=out_specs, check_vma=False)
```

```python
import functools
import math

import jax
import jax.numpy as jnp
from jax import lax
from jax.experimental import pallas as pl
from jax.experimental.pallas import tpu as pltpu
from jax.sharding import PartitionSpec as P

STEPS = 2
NY = 16
NZ = 8
TILES = 24
CHUNKS = (6, 6)
PAD = 64
VMEM_LIMIT = 16 * 1024 * 1024


flow_step = 0.05
coef_third = 0.75 * flow_step
coef_second = 8.0 * flow_step / 9.0
coef_first = 0.25 * flow_step
coef_mixed = 2.0 * flow_step / 9.0


def link_tile(links, direction, row, column):
    ref, slot = links
    at = ((direction * 3 + row) * 3 + column) * 2
    return ref[slot, at], ref[slot, at + 1]


def forward(links, direction, vector):
    out = []
    for row in range(3):
        real = imag = None
        for column in range(3):
            wr, wi = link_tile(links, direction, row, column)
            vr, vi = vector[column]
            re = wr * vr - wi * vi
            im = wr * vi + wi * vr
            real = re if real is None else real + re
            imag = im if imag is None else imag + im
        out.append((real, imag))
    return out


def backward(links, direction, vector):
    out = []
    for row in range(3):
        real = imag = None
        for column in range(3):
            wr, wi = link_tile(links, direction, column, row)
            vr, vi = vector[column]
            re = wr * vr + wi * vi
            im = wr * vi - wi * vr
            real = re if real is None else real + re
            imag = im if imag is None else imag + im
        out.append((real, imag))
    return out


def each(function, *vectors):
    return [
        tuple(function(*(vector[colour][part] for vector in vectors)) for part in range(2))
        for colour in range(3)
    ]


def tiles_of(ref, base):
    return [(ref[base + 2 * colour], ref[base + 2 * colour + 1]) for colour in range(3)]


def rows_of(ref, base):
    return [
        tuple(
            jnp.broadcast_to(ref[pl.ds(base + 2 * colour + part, 1), :], (8, 128))
            for part in range(2)
        )
        for colour in range(3)
    ]


def put_tiles(ref, base, vector):
    for colour in range(3):
        for part in range(2):
            ref[base + 2 * colour + part] = vector[colour][part]


def put_rows(ref, base, vector, row):
    for colour in range(3):
        for part in range(2):
            ref[pl.ds(base + 2 * colour + part, 1), :] = vector[colour][part][row : row + 1, :]


def roll(value, shift, axis):
    return pltpu.roll(value, shift % value.shape[axis], axis)


def messages(links, base, field, pulled_ref, low_ref, high_ref):
    put_tiles(pulled_ref, base, backward(links, 0, field))
    put_rows(low_ref, base, field, 0)
    put_rows(high_ref, base, backward(links, 1, field), 7)


def each_vector(columns):
    def loop(work):
        @pl.loop(0, columns)
        def _(column):
            for spin in range(4):
                work(spin, pl.multiple_of(column * TILES, TILES) + 6 * spin)

    return loop


def first_kernel(
    start, columns, index_ref, field_ref, links_ref, raw_ref, pulled_ref, slots_ref, next_ref, sems
):
    def copy_in(column):
        return pltpu.make_async_copy(
            field_ref.at[pl.ds((start + column) * TILES, TILES)],
            raw_ref.at[pl.ds(column * TILES, TILES)],
            sems.at[column],
        )

    index_copy = pltpu.make_async_copy(index_ref, slots_ref, sems.at[columns])
    link_copy = pltpu.make_async_copy(
        links_ref.at[:, pl.ds(0, 18)], next_ref, sems.at[columns + 1]
    )
    index_copy.start()
    link_copy.start()
    for column in range(columns):
        copy_in(column).start()
    index_copy.wait()
    link_copy.wait()
    links = (next_ref, slot_of(slots_ref, 0))

    @pl.loop(0, columns)
    def _(column):
        copy_in(column).wait()
        for spin in range(4):
            base = pl.multiple_of(column * TILES, TILES) + 6 * spin
            put_tiles(pulled_ref, base, backward(links, 0, tiles_of(raw_ref, base)))


def first_rows_kernel(sizes, index_ref, links_ref, *refs):
    links = (links_ref, slot_of(index_ref, 0))
    for chunk, columns in enumerate(sizes):
        raw_ref = refs[chunk]
        low_ref, high_ref = refs[len(sizes) + 2 * chunk : len(sizes) + 2 * chunk + 2]

        @each_vector(columns)
        def _(spin, base):
            field = tiles_of(raw_ref, base)
            put_rows(low_ref, base, field, 0)
            put_rows(high_ref, base, backward(links, 1, field), 7)


def local_terms(base, centre, right_ref, left_ref, links, masks, total):
    is_top, is_bottom, is_far, is_near = masks
    add = functools.partial(each, lambda a, b: a + b)
    above_x = each(
        lambda v, h: jnp.where(is_top, h, roll(v, -1, 0)), centre, rows_of(right_ref, base)
    )
    total = add(total, forward(links, 1, above_x))
    below_x = each(
        lambda v, h: jnp.where(is_bottom, h, roll(v, 1, 0)),
        backward(links, 1, centre),
        rows_of(left_ref, base),
    )
    total = add(total, below_x)
    total = add(total, forward(links, 2, each(lambda v: roll(v, -NZ, 1), centre)))
    total = add(total, each(lambda v: roll(v, NZ, 1), backward(links, 2, centre)))
    above_z = each(lambda v: jnp.where(is_far, roll(v, NZ - 1, 1), roll(v, -1, 1)), centre)
    total = add(total, forward(links, 3, above_z))
    below_z = each(
        lambda v: jnp.where(is_near, roll(v, 1 - NZ, 1), roll(v, 1, 1)),
        backward(links, 3, centre),
    )
    return add(total, below_z)


def edge_masks():
    sub = lax.broadcasted_iota(jnp.int32, (8, 128), 0)
    zcoord = lax.broadcasted_iota(jnp.int32, (8, 128), 1) % NZ
    return sub == 7, sub == 0, zcoord == NZ - 1, zcoord == 0


def lap_kernel(lap, columns, nx_total, index_ref, *refs):
    kind = lap % 3
    refs = list(refs)
    centre_ref, above_ref, below_ref, right_ref, left_ref, links_ref = refs[:6]
    refs = refs[6:]
    aux_ref = refs.pop(0) if kind > 0 else None
    if nx_total:
        source_ref, momenta_ref = refs[:2]
        refs = refs[2:]
        both_ref = refs.pop()
        phases(nx_total, source_ref, momenta_ref, refs.pop(), both_ref)
    out_ref = refs.pop(0)
    sum_ref = refs.pop(0) if kind == 1 else None
    pulled_ref, low_ref, high_ref = refs

    links = (links_ref, slot_of(index_ref, lap))
    links_next = (links_ref, slot_of(index_ref, lap + 1))
    masks = edge_masks()
    add = functools.partial(each, lambda a, b: a + b)

    @each_vector(columns)
    def _(spin, base):
        centre = tiles_of(centre_ref, base)
        total = each(lambda v, p: p - 8.0 * v, centre, tiles_of(below_ref, base))
        total = add(total, forward(links, 0, tiles_of(above_ref, base)))
        total = local_terms(base, centre, right_ref, left_ref, links, masks, total)
        if kind == 0:
            field = each(lambda t: coef_third * t, total)
        elif kind == 1:
            middle = each(lambda a, t: a + coef_second * t, tiles_of(aux_ref, base), total)
            field = each(lambda m, v: coef_first * m - coef_mixed * v, middle, centre)
            put_tiles(sum_ref, base, add(middle, centre))
        else:
            field = add(tiles_of(aux_ref, base), total)
        put_tiles(out_ref, base, field)
        messages(links_next, base, field, pulled_ref, low_ref, high_ref)


def local_kernel(
    lap, columns, index_ref, centre_ref, right_ref, left_ref, links_ref, aux_ref, out_ref
):
    links = (links_ref, slot_of(index_ref, lap))
    masks = edge_masks()

    @each_vector(columns)
    def _(spin, base):
        centre = tiles_of(centre_ref, base)
        total = each(lambda v, a: a - 8.0 * v, centre, tiles_of(aux_ref, base))
        total = local_terms(base, centre, right_ref, left_ref, links, masks, total)
        put_tiles(out_ref, base, total)


def final_kernel(lap, start, columns, last, scale, index_ref, *refs):
    refs = list(refs)
    partial_ref, above_ref, below_ref, links_ref, before_ref = refs[:5]
    table_ref = refs[5] if last else None
    out_ref, result_ref, held_ref, total_ref, sems = refs[-5:]
    links = (links_ref, slot_of(index_ref, lap))
    total_ref[...] = before_ref[...] if start else jnp.zeros((8, 128), jnp.float32)

    def copy_out(column):
        return pltpu.make_async_copy(
            held_ref.at[pl.ds(column * TILES, TILES)],
            out_ref.at[pl.ds((start + column) * TILES, TILES)],
            sems.at[column],
        )

    @pl.loop(0, columns)
    def _(column):
        density = total_ref[...]
        for spin in range(4):
            base = pl.multiple_of(column * TILES, TILES) + 6 * spin
            total = each(lambda a, b: a + b, tiles_of(partial_ref, base), tiles_of(below_ref, base))
            field = each(
                lambda a, b: a + b, total, forward(links, 0, tiles_of(above_ref, base))
            )
            put_tiles(held_ref, base, field)
            part = None
            for colour in range(3):
                for value in field[colour]:
                    part = value * value if part is None else part + value * value
            density = density + part if spin < 2 else density - part
        total_ref[...] = density
        copy_out(column).start()

    if last:
        sums = None
        for row in range(8):
            whole = jnp.broadcast_to(total_ref[row : row + 1, :], (128, 128))
            term = table_ref[pl.ds(row * 128, 128), :] * whole
            sums = term if sums is None else sums + term
        sums = lax.dot_general(
            jnp.full((8, 128), 1.0, jnp.float32),
            sums,
            (((1,), (1,)), ((), ())),
            precision=lax.Precision.HIGHEST,
            preferred_element_type=jnp.float32,
        )
        sums = sums * scale
        for row in range(result_ref.shape[0]):
            result_ref[row] = sums[0:1, :]
    else:
        result_ref[...] = total_ref[...]

    @pl.loop(0, columns)
    def _(column):
        copy_out(column).wait()


def phases(nx_total, source_ref, momenta_ref, table_ref, both_ref):
    count = momenta_ref.shape[1]
    both_ref[...] = jnp.zeros(both_ref.shape, jnp.int32)
    both_ref[0:3, 0:count] = momenta_ref[...]
    both = both_ref[...]
    both_ref[...] = both + roll(both, PAD, 1)
    sites = lax.broadcasted_iota(jnp.int32, (128, 128), 0)
    quarter = jnp.where(lax.broadcasted_iota(jnp.int32, (128, 128), 1) >= PAD, 0.25, 0.0)

    def within(value, size):
        return jnp.bitwise_and(value, size - 1)

    def fraction(axis, distance, size):
        momentum = jnp.broadcast_to(both_ref[axis : axis + 1, :], (128, 128))
        return within(momentum * within(distance, size), size).astype(jnp.float32) * (1.0 / size)

    plane = fraction(1, sites // NZ - source_ref[1], NY) + quarter
    plane = plane + fraction(2, within(sites, NZ) - source_ref[2], NZ)
    first = lax.axis_index("xyz") * 8

    @pl.loop(0, 8)
    def _(row):
        xcoord = jnp.full((128, 128), first + row - source_ref[0], jnp.int32)
        turns = plane + fraction(0, xcoord, nx_total)
        turns = turns - jnp.floor(turns)
        waves = jnp.cos(2.0 * math.pi * turns)
        table_ref[pl.ds(pl.multiple_of(row * 128, 128), 128), :] = waves.T


def total_kernel(all_ref, out_ref):
    count = out_ref.shape[2]
    total = jnp.sum(all_ref[...], axis=0)
    out_ref[0] = total[:, 0:count]
    out_ref[1] = total[:, PAD : PAD + count]


def slot_of(index, lap):
    return index[STEPS - 1 - lap // 3, 2 - lap % 3]


def shape(*dims):
    return jax.ShapeDtypeStruct(dims, jnp.float32)


def cost(columns, per_spin, arrays):
    return pl.CostEstimate(
        flops=columns * 4 * per_spin * 1024,
        bytes_accessed=columns * TILES * 4096 * arrays,
        transcendentals=0,
    )


def params():
    return pltpu.CompilerParams(vmem_limit_bytes=VMEM_LIMIT)


def whole_spec():
    return pl.BlockSpec(memory_space=pltpu.VMEM)


SMEM = pl.BlockSpec(memory_space=pltpu.SMEM)
VMEM = pl.BlockSpec(memory_space=pltpu.VMEM)
ANY = pl.BlockSpec(memory_space=pl.ANY)


def first_messages(index, links, field, start, columns):
    return pl.pallas_call(
        functools.partial(first_kernel, start, columns),
        in_specs=[ANY] * 3,
        out_specs=[VMEM] * 2,
        scratch_shapes=[
            pltpu.SMEM(index.shape, jnp.int32),
            pltpu.VMEM((links.shape[0], 18, 8, 128), jnp.float32),
            pltpu.SemaphoreType.DMA((columns + 2,)),
        ],
        out_shape=[shape(columns * TILES, 8, 128)] * 2,
        compiler_params=params(),
        cost_estimate=cost(columns, 70, 2),
        name="first_messages",
    )(*(pltpu.with_memory_space_constraint(a, pltpu.HBM) for a in (index, field, links)))


def first_rows(index, links, fields, sizes):
    shapes = [shape(columns * TILES, 128) for columns in sizes for _ in range(2)]
    return pl.pallas_call(
        functools.partial(first_rows_kernel, sizes),
        in_specs=[SMEM] + [VMEM] * (1 + len(fields)),
        out_specs=[VMEM] * len(shapes),
        out_shape=shapes,
        compiler_params=params(),
        cost_estimate=cost(sum(sizes), 70, 1),
        name="first_rows",
    )(index, links, *fields)


def lap_call(lap, index, links, centre, arrived, aux, columns, phase=None):
    kind = lap % 3
    operands = [index, centre, *arrived, links]
    if kind > 0:
        operands.append(aux)
    in_specs = [SMEM] + [VMEM] * (len(operands) - 1)
    fields = 3 if kind == 1 else 2
    out_shape = [shape(columns * TILES, 8, 128)] * fields + [shape(columns * TILES, 128)] * 2
    scratch, nx_total = [], 0
    if phase is not None:
        nx_total, source, momenta = phase
        operands += [source, momenta.T]
        in_specs += [SMEM, VMEM]
        out_shape.append(shape(8 * 128, 128))
        scratch = [pltpu.VMEM((8, 128), jnp.int32)]
    return pl.pallas_call(
        functools.partial(lap_kernel, lap, columns, nx_total),
        in_specs=in_specs,
        out_specs=[VMEM] * len(out_shape),
        scratch_shapes=scratch,
        out_shape=out_shape,
        compiler_params=params(),
        cost_estimate=cost(columns, 700, 6),
        name=f"lap{lap}_{columns}",
    )(*operands)


def local_call(lap, index, links, centre, right, left, aux, columns):
    return pl.pallas_call(
        functools.partial(local_kernel, lap, columns),
        in_specs=[SMEM] + [VMEM] * 5,
        out_specs=VMEM,
        out_shape=shape(columns * TILES, 8, 128),
        compiler_params=params(),
        cost_estimate=cost(columns, 450, 3),
        name=f"local{lap}_{columns}",
    )(index, centre, right, left, links, aux)


def final_call(lap, index, links, partial, above, below, before, table, start, columns, sizes, scale):
    every, told = sizes
    last = table is not None
    buffer, density = before
    operands = [index, partial, above, below, links, density]
    in_specs = [SMEM] + [VMEM] * 5
    if last:
        operands.append(table)
        in_specs.append(VMEM)
    aliases = {}
    if buffer is not None:
        aliases = {len(operands): 0}
        operands.append(buffer)
        in_specs.append(ANY)
    return pl.pallas_call(
        functools.partial(final_kernel, lap, start, columns, last, scale),
        in_specs=in_specs,
        out_specs=[ANY, VMEM],
        scratch_shapes=[
            pltpu.VMEM((columns * TILES, 8, 128), jnp.float32),
            pltpu.VMEM((8, 128), jnp.float32),
            pltpu.SemaphoreType.DMA((columns,)),
        ],
        out_shape=[
            shape(every * TILES, 8, 128),
            shape(told, 1, 128) if last else shape(8, 128),
        ],
        input_output_aliases=aliases,
        compiler_params=params(),
        cost_estimate=cost(columns, 100, 4),
        name=f"final{start}_{columns}",
    )(*operands)


def total_call(everything, count):
    return pl.pallas_call(
        total_kernel,
        in_specs=[VMEM],
        out_specs=VMEM,
        out_shape=shape(2, 1, count),
        compiler_params=params(),
        cost_estimate=pl.CostEstimate(flops=10_000, bytes_accessed=10_000, transcendentals=0),
        name="total",
    )(everything)


def passed_along(block, axis, distance):
    devices = range(lax.axis_size(axis))
    route = [((i - distance) % len(devices), i) for i in devices]
    return lax.ppermute(block, axis, route)


def exchanged(field, pulled, low, high):
    return (
        passed_along(field, "ta", -1),
        passed_along(pulled, "ta", 1),
        passed_along(low, "xyz", -1),
        passed_along(high, "xyz", 1),
    )


def body(sink, links, section_index, momenta, source):
    every = sink.shape[0]
    size = lax.axis_size("xyz")
    nx_total = sink.shape[5] * size
    whole_field = sink.reshape(every * TILES, 8, 128)
    links = links.reshape(links.shape[0], 72, 8, 128)
    laps = 3 * STEPS

    starts = [sum(CHUNKS[:i]) for i in range(len(CHUNKS))]
    made = [
        first_messages(section_index, links, whole_field, start, columns)
        for start, columns in zip(starts, CHUNKS)
    ]
    rows = first_rows(section_index, links, [raw for raw, _ in made], CHUNKS)
    state = [
        (raw, raw, exchanged(raw, pulled, *rows[2 * chunk : 2 * chunk + 2]))
        for chunk, (raw, pulled) in enumerate(made)
    ]
    table = None
    for lap in range(laps - 1):
        for chunk, columns in enumerate(CHUNKS):
            centre, aux, arrived = state[chunk]
            with_table = lap == 2 and chunk == len(CHUNKS) - 1
            phase = (nx_total, source, momenta) if with_table else None
            made = lap_call(lap, section_index, links, centre, arrived, aux, columns, phase)
            if with_table:
                *made, table = made
            field = made[0]
            if lap % 3 == 1:
                aux = made[1]
            elif lap % 3 == 2:
                aux = field
            state[chunk] = (field, aux, exchanged(field, *made[-3:]))

    scale = 1.0 / math.sqrt(576.0 * nx_total * NY * NZ)
    lap = laps - 1
    buffer, result = None, state[0][2][2]
    for chunk, (start, columns) in enumerate(zip(starts, CHUNKS)):
        centre, aux, (above, below, right, left) = state[chunk]
        partial = local_call(lap, section_index, links, centre, right, left, aux, columns)
        last = chunk == len(CHUNKS) - 1
        buffer, result = final_call(
            lap,
            section_index,
            links,
            partial,
            above,
            below,
            (buffer, result),
            table if last else None,
            start,
            columns,
            (every, size),
            scale,
        )
    everything = lax.all_to_all(result, "xyz", split_axis=0, concat_axis=0, tiled=True)
    correlator = total_call(everything, momenta.shape[0])
    return (buffer.reshape(sink.shape), correlator.reshape(2, momenta.shape[0], 1))


def solution(mesh):
    in_specs = (
        P("cfg", None, None, None, "ta", "xyz", None),
        P("cfg", None, None, None, None, "ta", "xyz", None),
        P(),
        P(),
        P(),
    )
    out_specs = (P("cfg", None, None, None, "ta", "xyz", None), P("cfg", None, "ta"))
    return jax.shard_map(body, mesh=mesh, in_specs=in_specs, out_specs=out_specs, check_vma=False)
```
